8 devices in a mesh: dp: 2 (over z, y), sp: 4 (over x, core).
Axes of the slice: x: 2, y: 2, z: 1, core: 2. Of those that a mesh axis runs over, the one named last changes fastest.
Arguments:
- feature_map: bfloat16 [400, 336, 256], P(('dp', 'sp')), parts along dimension 0
- box_coords: int32 [2048, 4], P('dp'), parts along dimension 0
- w_one: bfloat16 [12544, 1024], replicated
- b_one: float32 [1024], replicated
- w_two: bfloat16 [1024, 1024], replicated
- b_two: float32 [1024], replicated
Outputs:
- output: bfloat16 [2048, 1024], P(('dp', 'sp')), parts along dimension 0
There are 2 independent parts. The reference program is written for one: setup_inputs(seed, part) draws one part's arguments, and reference() takes and returns one part's arrays. A program takes and returns all parts, laid end to end along the dimension named above; an argument that names none is the same for every part.
All inputs are finite; a program needn't handle non-finite values.
Results may differ from the reference program's by a relative error of at most 0.00712392.
Values are sent between devices in bfloat16 or wider.
A program may use at most 1 GiB of HBM per device.

```python
import jax
import jax.numpy as jnp
from jax import lax

FEAT_H = 200
FEAT_W = 336
CHANNELS = 256
HIDDEN = 1024
GROUP_SIZE = 4
ROIS_DEV = 256
POOL_BINS = 7
TILE_ROWS = FEAT_H // GROUP_SIZE
REGIONS = ROIS_DEV * GROUP_SIZE
HEAD_IN = POOL_BINS * POOL_BINS * CHANNELS
SPAN_LOW = (8 * TILE_ROWS + 6) // 7
SPAN_HIGH = (24 * TILE_ROWS - 16) // 7
WIDTH_LOW = POOL_BINS + 1
WIDTH_HIGH = (8 * FEAT_W) // 14


def bin_weights(start_eighths, span_units, length, offset, num_rows):
    sample_ids = jnp.arange(2 * POOL_BINS, dtype=jnp.int32)
    sample_pos = 4 * start_eighths[..., None] - 16 + (2 * sample_ids + 1) * span_units[..., None]
    inside = (sample_pos >= -32) & (sample_pos <= 32 * length)
    sample_pos = jnp.maximum(sample_pos, 0)
    low_row = sample_pos // 32
    frac_part = sample_pos % 32
    at_top = low_row >= length - 1
    low_row = jnp.where(at_top, length - 1, low_row)
    frac_part = jnp.where(at_top, 0, frac_part)
    low_wt = jnp.where(inside, 32 - frac_part, 0)
    high_wt = jnp.where(inside, frac_part, 0)
    grid_rows = offset + jnp.arange(num_rows, dtype=jnp.int32)
    weights = (grid_rows == low_row[..., None]) * low_wt[..., None] + (grid_rows == low_row[..., None] + 1) * high_wt[..., None]
    weights = weights.reshape(weights.shape[:-2] + (POOL_BINS, 2, num_rows)).sum(axis=-2)
    return (weights.astype(jnp.float32) / 64.0).astype(jnp.bfloat16)


def draw_boxes(key):
    subkeys = jax.random.split(key, 7)
    region_ids = jnp.arange(REGIONS)
    span_y = jax.random.randint(subkeys[0], (REGIONS,), SPAN_LOW, SPAN_HIGH + 1)
    span_y = jnp.where(region_ids == 0, SPAN_HIGH, jnp.where(region_ids == 1, SPAN_LOW, span_y))
    height_units = 7 * span_y
    spread_y = jax.random.randint(subkeys[1], (REGIONS,), 0, 8 * FEAT_H - height_units + 1)
    hot_center = jax.random.randint(subkeys[2], (), 0, 8 * FEAT_H)
    jitter = jax.random.randint(subkeys[3], (REGIONS,), -8 * TILE_ROWS, 8 * TILE_ROWS + 1)
    near_y = jnp.clip(hot_center - height_units // 2 + jitter, 0, 8 * FEAT_H - height_units)
    pick_near = jax.random.randint(subkeys[4], (REGIONS,), 0, 2)
    top_y = jnp.where(pick_near == 1, near_y, spread_y)
    span_x = jax.random.randint(subkeys[5], (REGIONS,), WIDTH_LOW, WIDTH_HIGH + 1)
    span_x = jnp.where(region_ids == 0, WIDTH_HIGH, jnp.where(region_ids == 1, WIDTH_LOW, span_x))
    width_units = 7 * span_x
    left_x = jax.random.randint(subkeys[6], (REGIONS,), 0, 8 * FEAT_W - width_units + 1)
    return jnp.stack([top_y, left_x, top_y + height_units, left_x + width_units], axis=1).astype(jnp.int32)


def setup_inputs(seed: int = 0, part: int = 0) -> dict:
    part_key = jax.random.fold_in(jax.random.key(seed), part)
    key_noise, key_chan, key_row, key_box = jax.random.split(part_key, 4)
    feat_noise = jax.random.normal(key_noise, (FEAT_H, FEAT_W, CHANNELS), jnp.float32)
    chan_mean = 0.5 + 0.3 * jax.random.normal(key_chan, (CHANNELS,), jnp.float32)
    row_trend = 0.5 * jax.random.normal(key_row, (FEAT_H,), jnp.float32)
    feature_map = (feat_noise + chan_mean[None, None, :] + row_trend[:, None, None]).astype(jnp.bfloat16)
    box_coords = draw_boxes(key_box)
    key_w1, key_b1, key_w2, key_b2 = jax.random.split(jax.random.key(seed + 1), 4)
    w_one = (jax.random.normal(key_w1, (HEAD_IN, HIDDEN), jnp.float32) * HEAD_IN ** -0.5).astype(jnp.bfloat16)
    b_one = 0.5 * jax.random.normal(key_b1, (HIDDEN,), jnp.float32)
    w_two = (jax.random.normal(key_w2, (HIDDEN, HIDDEN), jnp.float32) * (2.0 / HIDDEN) ** 0.5).astype(jnp.bfloat16)
    b_two = 0.5 * jax.random.normal(key_b2, (HIDDEN,), jnp.float32)
    return {'feature_map': feature_map, 'box_coords': box_coords, 'w_one': w_one, 'b_one': b_one, 'w_two': w_two, 'b_two': b_two}


def reference(feature_map, box_coords, w_one, b_one, w_two, b_two):
    span_y = (box_coords[:, 2] - box_coords[:, 0]) // 7
    span_x = (box_coords[:, 3] - box_coords[:, 1]) // 7
    col_wts = bin_weights(box_coords[:, 1], span_x, FEAT_W, 0, FEAT_W).reshape(REGIONS * POOL_BINS, FEAT_W)
    tile_stack = feature_map.reshape(GROUP_SIZE, TILE_ROWS, FEAT_W, CHANNELS)

    def add_tile(running, step_in):
        tile_feat, tile_id = step_in
        row_wts = bin_weights(box_coords[:, 0], span_y, FEAT_H, tile_id * TILE_ROWS, TILE_ROWS)
        tile_mat = tile_feat.transpose(1, 0, 2).reshape(FEAT_W, TILE_ROWS * CHANNELS)
        across = jnp.dot(col_wts, tile_mat, preferred_element_type=jnp.float32)
        across = across.reshape(REGIONS, POOL_BINS, TILE_ROWS, CHANNELS)
        tile_part = jnp.einsum('rih,rjhc->rijc', row_wts.astype(jnp.float32), across)
        return running + tile_part.astype(jnp.bfloat16).astype(jnp.float32), None

    start_sum = jnp.zeros((REGIONS, POOL_BINS, POOL_BINS, CHANNELS), jnp.float32)
    pooled_sum = lax.scan(add_tile, start_sum, (tile_stack, jnp.arange(GROUP_SIZE, dtype=jnp.int32)))[0]
    pooled = pooled_sum.astype(jnp.bfloat16).reshape(REGIONS, HEAD_IN)
    hidden_act = jnp.maximum(jnp.dot(pooled, w_one, preferred_element_type=jnp.float32) + b_one, 0.0).astype(jnp.bfloat16)
    head_out = jnp.maximum(jnp.dot(hidden_act, w_two, preferred_element_type=jnp.float32) + b_two, 0.0).astype(jnp.bfloat16)
    return head_out
```

```python
import functools

import jax
import jax.numpy as jnp
from jax import lax
from jax.experimental import pallas as pl
from jax.experimental.pallas import tpu as pltpu
from jax.sharding import PartitionSpec as P

BINS = 7
SAMPLES = 2 * BINS
HALO = 6
WINDOW = 256
BLOCK = 16
SLOTS = 11


def sample_rows(start_eighths, span_units, length):
    ids = jnp.arange(SAMPLES, dtype=jnp.int32)
    pos = 4 * start_eighths[..., None] - 16 + (2 * ids + 1) * span_units[..., None]
    inside = (pos >= -32) & (pos <= 32 * length)
    return pos, inside


def column_table(boxes, feat_w):
    pos, inside = sample_rows(boxes[..., 1], (boxes[..., 3] - boxes[..., 1]) // 7, feat_w)
    pos = jnp.clip(pos, 0, 32 * (feat_w - 1))
    right = pos[..., 0] // 32 >= feat_w - WINDOW
    shift = jnp.where(right, feat_w - WINDOW, 0)
    at = (pos - 32 * shift[..., None]).astype(jnp.float32) / 32.0
    gain = jnp.where(inside, 0.5, 0.0)
    pad = [(0, 0)] * (at.ndim - 1) + [(0, 1)]
    cols = lax.broadcasted_iota(jnp.float32, at.shape[:-1] + (BINS + 1, WINDOW), at.ndim)

    def tent(which):
        x = jnp.pad(at[..., which::2], pad)[..., None]
        g = jnp.pad(gain[..., which::2], pad)[..., None]
        return jnp.maximum(1.0 - jnp.abs(cols - x), 0.0) * g

    return tent(0) + tent(1), right


def row_lists(boxes, right, chip, tile_rows, length):
    regions = boxes.shape[-2]
    chip_rows = 2 * tile_rows
    lists = chip_rows + HALO - 1
    width = regions + 2 * BLOCK
    pos, inside = sample_rows(boxes[..., 0], (boxes[..., 2] - boxes[..., 0]) // 7, length)
    pos = jnp.maximum(pos, 0)
    at_top = pos // 32 >= length - 1
    low = jnp.where(at_top, length - 2, pos // 32)
    frac = jnp.where(at_top, 32, pos % 32)
    first, last = low[..., 0::2], low[..., 1::2] + 1
    owned = (first + last) // 2 // chip_rows == chip
    tile = first // tile_rows
    straddle = owned & (last // tile_rows > tile)
    edge = (tile + 1) * tile_rows
    parity = tile % 2

    def per_sample(a):
        return jnp.repeat(a, 2, axis=-1)

    ids = jnp.arange(regions, dtype=jnp.int32)[:, None]
    bin_slot = 1 + jnp.arange(SAMPLES, dtype=jnp.int32) // 2
    part_slot = 1 + BINS + per_sample(parity)
    upper = per_sample(straddle) & (low >= per_sample(edge))
    split = per_sample(straddle) & (low == per_sample(edge) - 1)
    live = per_sample(owned) & inside
    start = chip * (chip_rows - HALO)
    head = frac + (ids << 18)
    code_one = head + ((ids * SLOTS + jnp.where(upper, part_slot, bin_slot)) << 6)
    code_two = head + ((ids * SLOTS + part_slot) << 6)
    list_one = jnp.where(live, low - start, -1)
    list_two = jnp.where(live & split, lists + per_sample(tile) - chip, -1)
    list_ids = jnp.arange(lists + 2, dtype=jnp.int32)[:, None]
    lo = jnp.moveaxis(list_one, -1, 0)[..., None, :]
    hi = jnp.moveaxis(list_two, -1, 0)[..., None, :]
    co = jnp.moveaxis(code_one, -1, 0)[..., None, :]
    ch = jnp.moveaxis(code_two, -1, 0)[..., None, :]
    code = jnp.sum(jnp.where(lo == list_ids, co, 0) + jnp.where(hi == list_ids, ch, 0), axis=0)
    touch = jnp.sum((lo == list_ids).astype(jnp.int32) + (hi == list_ids).astype(jnp.int32), axis=0) > 0

    is_right = right[..., None, :]
    kinds = jnp.stack([touch & ~is_right, touch & is_right])
    before = (jnp.arange(regions)[:, None] < jnp.arange(regions)[None, :]).astype(jnp.bfloat16)
    rank = jnp.einsum('tgvr,rs->tgvs', kinds.astype(jnp.bfloat16), before, preferred_element_type=jnp.float32).astype(jnp.int32)
    place = jnp.where(is_right, width - 1 - rank[1], rank[0])
    place = jnp.where(touch, place, -1)
    count = jnp.sum(kinds.astype(jnp.int32), axis=-1)
    seats = jnp.arange(width, dtype=jnp.int32)
    table = jnp.sum(jnp.where(place[..., :, None] == seats, code[..., :, None], 0), axis=-2)
    table = jnp.pad(table, ((0, 0), (0, 1), (0, 0)))

    blocks = (jnp.moveaxis(count, 0, -1).reshape(count.shape[1], -1) + BLOCK - 1) // BLOCK
    order = jnp.arange(blocks.shape[-1], dtype=jnp.int32)
    upto = jnp.sum(jnp.where(order[:, None] <= order[None, :], blocks[:, :, None], 0), axis=1)
    total = upto[:, -1]
    most = (regions * (SAMPLES + 2) + (BLOCK - 1) * blocks.shape[-1]) // BLOCK + 4
    turn = jnp.arange(most, dtype=jnp.int32) - 1
    which = jnp.sum((upto[:, None, :] <= turn[:, None]).astype(jnp.int32), axis=-1)
    nth = turn - jnp.sum(jnp.where(order < which[..., None], blocks[:, None, :], 0), axis=-1)
    kind = which % 2
    base = jnp.where(kind == 1, width - BLOCK * (nth + 1), BLOCK * nth)
    real = (turn >= 0) & (turn < total[:, None])
    plan = jnp.where(real, which // 2 + (kind << 8) + (base << 9), lists + 2)

    edges = (jnp.arange(2, dtype=jnp.int32) + 1 + chip) * tile_rows - 1 - start
    every = jnp.arange(lists, dtype=jnp.int32)
    row_of = jnp.concatenate([every, edges, jnp.zeros((1,), jnp.int32)])
    on_edge = (every == edges[0]) | (every == edges[1])
    low_gain = jnp.concatenate([jnp.full((lists,), 1 / 64), jnp.zeros((3,))]).astype(jnp.float32)
    high_gain = jnp.concatenate([jnp.where(on_edge, 0.0, 1 / 64), jnp.full((2,), 1 / 64), jnp.zeros((1,))]).astype(jnp.float32)

    bins = jnp.arange(BINS, dtype=jnp.int32) + 1
    joins = jnp.stack([jnp.sum(jnp.where(straddle & (parity == q), bins, 0), axis=-1) for q in range(2)], axis=-1)
    return table.reshape(table.shape[0], -1), plan, total, row_of, low_gain, high_gain, joins.reshape(joins.shape[0], -1)


def pool_kernel(dims, list_ref, plan_ref, meta_ref, row_ref, low_ref, high_ref, join_ref, tab_ref, own_ref, mate_ref, halo_ref, w_ref, out_ref,
                feat, acc_a, acc_b, lhs, wbuf, out_one, out_two, fsem, wsem):
    tile_rows, feat_w, channels, regions, width = dims
    chip, core, total = meta_ref[0], meta_ref[1], meta_ref[2]
    half = channels // 2
    row_in = BINS * channels
    first = chip * HALO
    copies = [
        pltpu.make_async_copy(own_ref, feat.at[pl.ds(first + core * tile_rows, tile_rows)], fsem.at[0]),
        pltpu.make_async_copy(mate_ref, feat.at[pl.ds(first + (1 - core) * tile_rows, tile_rows)], fsem.at[1]),
        pltpu.make_async_copy(halo_ref, feat.at[pl.ds((1 - chip) * 2 * tile_rows, HALO)], fsem.at[2]),
    ]
    for copy in copies:
        copy.start()
    depth = wbuf.shape[0]

    def weights(i):
        return pltpu.make_async_copy(w_ref.at[pl.ds(i * row_in, row_in)], wbuf.at[i % depth], wsem.at[i % depth])

    for i in range(depth):
        weights(i).start()

    zero = jnp.zeros((8 * SLOTS, half), jnp.float32)

    def clear(r, _):
        at = pl.ds(pl.multiple_of(r * 8 * SLOTS, 8), 8 * SLOTS)
        acc_a[at, :] = zero
        acc_b[at, :] = zero
        return 0

    lax.fori_loop(0, regions, clear, 0)
    for copy in copies:
        copy.wait()

    def multiply(turn, out):
        plan = plan_ref[turn]
        v = plan & 255
        column = pl.multiple_of(((plan >> 8) & 1) * (feat_w - WINDOW), 16)
        at = v * width + (plan >> 9)
        rows = [tab_ref[list_ref[at + s] >> 18] for s in range(BLOCK)]
        left = jnp.concatenate(rows, axis=0).astype(jnp.bfloat16)
        row = row_ref[v]
        out[0] = jnp.dot(left, feat[row, pl.ds(column, WINDOW), :], preferred_element_type=jnp.float32)
        out[1] = jnp.dot(left, feat[row + 1, pl.ds(column, WINDOW), :], preferred_element_type=jnp.float32)

    def spread(turn, out):
        plan = plan_ref[turn]
        v = plan & 255
        at = v * width + (plan >> 9)
        low, high = low_ref[v], high_ref[v]
        for s0 in range(0, BLOCK, 4):
            slots, news = [], []
            for s in range(s0, s0 + 4):
                code = list_ref[at + s]
                frac = (code & 63).astype(jnp.float32)
                wl, wh = (32.0 - frac) * low, frac * high
                slot = pl.ds(pl.multiple_of(((code >> 6) & 4095) * 8, 8), 8)
                slots.append(slot)
                news.append((
                    acc_a[slot, :] + (out[0, 8 * s:8 * s + 8, :half] * wl + out[1, 8 * s:8 * s + 8, :half] * wh),
                    acc_b[slot, :] + (out[0, 8 * s:8 * s + 8, half:] * wl + out[1, 8 * s:8 * s + 8, half:] * wh),
                ))
            for slot, (a, b) in zip(slots, news):
                acc_a[slot, :] = a
                acc_b[slot, :] = b

    def pair(u, _):
        multiply(2 * u + 1, out_one)
        spread(2 * u, out_two)
        multiply(2 * u + 2, out_two)
        spread(2 * u + 1, out_one)
        return 0

    pairs = (total + 1) // 2
    out_two[...] = jnp.zeros_like(out_two)
    lax.fori_loop(0, pairs, pair, 0)
    spread(2 * pairs, out_two)

    def join(r, _):
        for q in range(2):
            to = pl.ds(pl.multiple_of((r * SLOTS + join_ref[2 * r + q]) * 8, 8), 8)
            part = pl.ds(pl.multiple_of((r * SLOTS + 1 + BINS + q) * 8, 8), 8)
            for acc in (acc_a, acc_b):
                acc[to, :] = acc[to, :].astype(jnp.bfloat16).astype(jnp.float32) + acc[part, :].astype(jnp.bfloat16).astype(jnp.float32)
        return 0

    lax.fori_loop(0, regions, join, 0)

    for i in range(BINS):
        for j in range(BINS):
            rows = pl.ds((1 + i) * 8 + j, regions, stride=8 * SLOTS)
            lhs[i % 2, :, j * channels:j * channels + half] = acc_a[rows, :].astype(jnp.bfloat16)
            lhs[i % 2, :, j * channels + half:(j + 1) * channels] = acc_b[rows, :].astype(jnp.bfloat16)
        weights(i).wait()
        part = jnp.dot(lhs[i % 2], wbuf[i % depth], preferred_element_type=jnp.float32)
        if i == 0:
            out_ref[...] = part
        else:
            out_ref[...] += part
        if i + depth < BINS:
            weights(i + depth).start()


def pool_and_project(lists, plan, meta, row_of, low_gain, high_gain, joins, tab, own, mate, halo, w_one):
    tile_rows, feat_w, channels = own.shape
    regions = tab.shape[0]
    hidden = w_one.shape[1]
    row_in = BINS * channels
    depth = 3
    dims = (tile_rows, feat_w, channels, regions, regions + 2 * BLOCK)
    smem = pl.BlockSpec(memory_space=pltpu.SMEM)
    vmem = pl.BlockSpec(memory_space=pltpu.VMEM)
    hbm = pl.BlockSpec(memory_space=pl.ANY)
    return pl.pallas_call(
        functools.partial(pool_kernel, dims),
        out_shape=jax.ShapeDtypeStruct((regions, hidden), jnp.float32),
        in_specs=[smem] * 7 + [vmem] + [hbm] * 4,
        out_specs=vmem,
        scratch_shapes=[
            pltpu.VMEM((2 * tile_rows + HALO, feat_w, channels), jnp.bfloat16),
            pltpu.VMEM((regions * SLOTS * 8, channels // 2), jnp.float32),
            pltpu.VMEM((regions * SLOTS * 8, channels // 2), jnp.float32),
            pltpu.VMEM((2, regions, row_in), jnp.bfloat16),
            pltpu.VMEM((depth, row_in, hidden), jnp.bfloat16),
            pltpu.VMEM((2, BLOCK * 8, channels), jnp.float32),
            pltpu.VMEM((2, BLOCK * 8, channels), jnp.float32),
            pltpu.SemaphoreType.DMA((3,)),
            pltpu.SemaphoreType.DMA((depth,)),
        ],
        compiler_params=pltpu.CompilerParams(vmem_limit_bytes=64 * 1024 * 1024 - 65536),
        cost_estimate=pl.CostEstimate(flops=30_000_000_000, bytes_accessed=50_000_000, transcendentals=0),
        name='pool',
    )(lists, plan, meta, row_of, low_gain, high_gain, joins, tab, own, mate, halo, w_one)


def solution(mesh):
    group = mesh.shape['sp']

    def device_step(feature_map, box_coords, w_one, b_one, w_two, b_two):
        tile_rows, feat_w, channels = feature_map.shape
        regions = box_coords.shape[0] // group
        me = lax.axis_index('sp')
        chip, core = me // 2, me % 2

        mate = lax.ppermute(feature_map, 'sp', [(0, 1), (1, 0), (2, 3), (3, 2)])
        rim = jnp.where(core == 1, feature_map[tile_rows - HALO:], feature_map[:HALO])
        hop_one = lax.ppermute(rim, 'sp', [(1, 2), (2, 1)])
        hop_two = lax.ppermute(hop_one, 'sp', [(1, 0), (2, 3)])
        halo = jnp.where((me == 1) | (me == 2), hop_one, hop_two)

        far = (me + 2) % 4
        boxes = jnp.stack([lax.dynamic_slice_in_dim(box_coords, g * regions, regions, 0) for g in (far, me)])
        tab, right = column_table(boxes, feat_w)
        lists, plan, total, row_of, low_gain, high_gain, joins = row_lists(boxes, right, chip, tile_rows, tile_rows * group)

        def project(g):
            meta = jnp.stack([chip, core, total[g]])
            return pool_and_project(lists[g], plan[g], meta, row_of, low_gain, high_gain, joins[g], tab[g], feature_map, mate, halo, w_one)

        away = project(0)
        back = lax.ppermute(away, 'sp', [(0, 2), (2, 0), (1, 3), (3, 1)])
        here = project(1)
        hidden_act = jnp.maximum(here + back + b_one, 0.0).astype(jnp.bfloat16)
        return jnp.maximum(jnp.dot(hidden_act, w_two, preferred_element_type=jnp.float32) + b_two, 0.0).astype(jnp.bfloat16)

    return jax.shard_map(device_step, mesh=mesh, in_specs=(P(('dp', 'sp'), None, None), P('dp', None), P(), P(), P(), P()), out_specs=P(('dp', 'sp'), None), check_vma=False)
```

```python
import functools

import jax
import jax.numpy as jnp
from jax import lax
from jax.experimental import pallas as pl
from jax.experimental.pallas import tpu as pltpu
from jax.sharding import PartitionSpec as P

BINS = 7
SAMPLES = 2 * BINS
HALO = 6
WINDOW = 256
BLOCK = 16
SLOTS = 11


def sample_rows(start_eighths, span_units, length):
    ids = jnp.arange(SAMPLES, dtype=jnp.int32)
    pos = 4 * start_eighths[..., None] - 16 + (2 * ids + 1) * span_units[..., None]
    inside = (pos >= -32) & (pos <= 32 * length)
    return pos, inside


def column_table(boxes, feat_w):
    pos, inside = sample_rows(boxes[..., 1], (boxes[..., 3] - boxes[..., 1]) // 7, feat_w)
    pos = jnp.clip(pos, 0, 32 * (feat_w - 1))
    right = pos[..., 0] // 32 >= feat_w - WINDOW
    shift = jnp.where(right, feat_w - WINDOW, 0)
    at = (pos - 32 * shift[..., None]).astype(jnp.float32) / 32.0
    gain = jnp.where(inside, 0.5, 0.0)
    pad = [(0, 0)] * (at.ndim - 1) + [(0, 1)]
    cols = lax.broadcasted_iota(jnp.float32, at.shape[:-1] + (BINS + 1, WINDOW), at.ndim)

    def tent(which):
        x = jnp.pad(at[..., which::2], pad)[..., None]
        g = jnp.pad(gain[..., which::2], pad)[..., None]
        return jnp.maximum(1.0 - jnp.abs(cols - x), 0.0) * g

    return tent(0) + tent(1), right


def row_lists(boxes, right, chip, tile_rows, length):
    regions = boxes.shape[-2]
    chip_rows = 2 * tile_rows
    lists, codes, plans = list_sizes(regions, tile_rows)
    pos, inside = sample_rows(boxes[..., 0], (boxes[..., 2] - boxes[..., 0]) // 7, length)
    pos = jnp.maximum(pos, 0)
    at_top = pos // 32 >= length - 1
    low = jnp.where(at_top, length - 2, pos // 32)
    frac = jnp.where(at_top, 32, pos % 32)
    first, last = low[..., 0::2], low[..., 1::2] + 1
    owned = (first + last) // 2 // chip_rows == chip
    tile = first // tile_rows
    straddle = owned & (last // tile_rows > tile)

    def per_sample(a):
        return jnp.repeat(a, 2, axis=-1)

    edge = per_sample((tile + 1) * tile_rows)
    part_slot = 1 + BINS + per_sample(tile % 2)
    upper = per_sample(straddle) & (low >= edge)
    split = per_sample(straddle) & (low == edge - 1)
    start = chip * (chip_rows - HALO)
    side = right[..., None].astype(jnp.int32)
    live = per_sample(owned) & inside
    slot = jnp.where(upper, part_slot, 1 + jnp.arange(SAMPLES, dtype=jnp.int32) // 2)
    ids = jnp.arange(regions, dtype=jnp.int32)[:, None]
    keys = frac + (slot << 6) + (ids << 10) + ((2 * jnp.where(live, low - start, lists) + side) << 18)
    extra = []
    for q in range(2):
        here = split & live & per_sample(tile % 2 == q)
        number = lists - 2 + (q - chip) % 2
        key = jnp.max(jnp.where(here, frac + ((1 + BINS + q) << 6) + (ids << 10) + ((2 * number + side) << 18), -1), axis=-1)
        extra.append(jnp.where(key < 0, (2 * lists) << 18, key))
    keys = jnp.concatenate([keys, jnp.stack(extra, axis=-1)], axis=-1)
    keys = jnp.sort(keys.reshape(keys.shape[0], -1), axis=-1)
    region = (keys >> 10) & 255
    code = (region * SLOTS + ((keys >> 6) & 15)) * 8 + (region << 15) + ((keys & 63) << 23)
    code = jnp.pad(code, ((0, 0), (0, codes - code.shape[-1])))

    order = jnp.arange(2 * lists + 1, dtype=jnp.int32)
    ahead = jnp.sum((keys[:, None, :] < (order << 18)[:, None]).astype(jnp.int32), axis=-1)
    begin, count = ahead[:, :-1], ahead[:, 1:] - ahead[:, :-1]
    blocks = (count + BLOCK - 1) // BLOCK
    order = order[:-1]
    prior = jnp.sum(jnp.where(order[:, None] < order[None, :], blocks[:, :, None], 0), axis=1)
    turn = jnp.arange(plans, dtype=jnp.int32)[:, None] - 1
    nth = turn - prior[:, None, :]
    packed = order + (jnp.minimum(count[:, None, :] - BLOCK * nth, BLOCK) << 8) + ((begin[:, None, :] + BLOCK * nth) << 13)
    plan = jnp.sum(jnp.where((nth >= 0) & (nth < blocks[:, None, :]), packed, 0), axis=-1)
    total = jnp.sum(blocks, axis=-1)

    bins = jnp.arange(BINS, dtype=jnp.int32) + 1
    joins = jnp.stack([jnp.sum(jnp.where(straddle & (tile % 2 == q), bins, 0), axis=-1) for q in range(2)], axis=-1)
    return code.reshape(-1), plan.reshape(-1), total, joins.reshape(-1)


def list_sizes(regions, tile_rows):
    lists = 2 * tile_rows + HALO - 1 + 2
    codes = regions * (SAMPLES + 2) + BLOCK
    plans = (regions * (SAMPLES + 2) + (BLOCK - 1) * 2 * lists) // BLOCK + 8
    return lists, codes, plans


def pool_kernel(dims, code_ref, plan_ref, total_ref, join_ref, tab_ref, own_ref, mate_ref, halo_ref, w_ref, out_ref,
                feat, acc_a, acc_b, lhs, wbuf, out_one, out_two, fsem, wsem):
    group, tile_rows, feat_w, channels, regions = dims
    lists, codes, plans = list_sizes(regions, tile_rows)
    me = lax.axis_index('sp')
    chip, core, total = me // 2, me % 2, total_ref[group]
    edge_one = tile_rows - 1 + chip * (tile_rows - 2 * tile_rows + HALO)
    edge_two = edge_one + tile_rows
    half = channels // 2
    row_in = BINS * channels
    first = chip * HALO
    copies = [
        pltpu.make_async_copy(own_ref, feat.at[pl.ds(first + core * tile_rows, tile_rows)], fsem.at[0]),
        pltpu.make_async_copy(mate_ref, feat.at[pl.ds(first + (1 - core) * tile_rows, tile_rows)], fsem.at[1]),
        pltpu.make_async_copy(halo_ref, feat.at[pl.ds((1 - chip) * 2 * tile_rows, HALO)], fsem.at[2]),
    ]
    for copy in copies:
        copy.start()
    depth = wbuf.shape[0]

    def weights(i):
        return pltpu.make_async_copy(w_ref.at[pl.ds(i * row_in, row_in)], wbuf.at[i % depth], wsem.at[i % depth])

    for i in range(depth):
        weights(i).start()

    zero = jnp.zeros((8 * SLOTS, half), jnp.float32)

    def clear(r, _):
        at = pl.ds(pl.multiple_of(r * 8 * SLOTS, 8), 8 * SLOTS)
        acc_a[at, :] = zero
        acc_b[at, :] = zero
        return 0

    lax.fori_loop(0, regions, clear, 0)
    for copy in copies:
        copy.wait()

    def multiply(turn, out):
        plan = plan_ref[group * plans + turn]
        v = (plan & 255) >> 1
        column = pl.multiple_of((plan & 1) * (feat_w - WINDOW), 16)
        at = group * codes + (plan >> 13)
        rows = [tab_ref[(code_ref[at + s] >> 15) & 255] for s in range(BLOCK)]
        left = jnp.concatenate(rows, axis=0).astype(jnp.bfloat16)
        row = jnp.where(v < lists - 2, v, jnp.where(v == lists - 2, edge_one, edge_two))
        out[0] = jnp.dot(left, feat[row, pl.ds(column, WINDOW), :], preferred_element_type=jnp.float32)
        out[1] = jnp.dot(left, feat[row + 1, pl.ds(column, WINDOW), :], preferred_element_type=jnp.float32)

    def spread(turn, out):
        plan = plan_ref[group * plans + turn]
        v = (plan & 255) >> 1
        live = (plan >> 8) & 31
        at = group * codes + (plan >> 13)
        low = jnp.where(v < lists - 2, 1 / 64, 0.0)
        high = jnp.where((v == edge_one) | (v == edge_two), 0.0, 1 / 64)
        for s0 in range(0, BLOCK, 4):
            slots, news = [], []
            for s in range(s0, s0 + 4):
                code = jnp.where(s < live, code_ref[at + s], 0)
                frac = (code >> 23).astype(jnp.float32)
                wl, wh = (32.0 - frac) * low, frac * high
                slot = pl.ds(pl.multiple_of(code & 32767, 8), 8)
                slots.append(slot)
                news.append((
                    acc_a[slot, :] + (out[0, 8 * s:8 * s + 8, :half] * wl + out[1, 8 * s:8 * s + 8, :half] * wh),
                    acc_b[slot, :] + (out[0, 8 * s:8 * s + 8, half:] * wl + out[1, 8 * s:8 * s + 8, half:] * wh),
                ))
            for slot, (a, b) in zip(slots, news):
                acc_a[slot, :] = a
                acc_b[slot, :] = b

    def pair(u, _):
        multiply(2 * u + 1, out_one)
        spread(2 * u, out_two)
        multiply(2 * u + 2, out_two)
        spread(2 * u + 1, out_one)
        return 0

    pairs = (total + 1) // 2
    out_two[...] = jnp.zeros_like(out_two)
    lax.fori_loop(0, pairs, pair, 0)
    spread(2 * pairs, out_two)

    def join(r, _):
        for q in range(2):
            to = pl.ds(pl.multiple_of((r * SLOTS + join_ref[(group * regions + r) * 2 + q]) * 8, 8), 8)
            part = pl.ds(pl.multiple_of((r * SLOTS + 1 + BINS + q) * 8, 8), 8)
            for acc in (acc_a, acc_b):
                acc[to, :] = acc[to, :].astype(jnp.bfloat16).astype(jnp.float32) + acc[part, :].astype(jnp.bfloat16).astype(jnp.float32)
        return 0

    lax.fori_loop(0, regions, join, 0)

    for i in range(BINS):
        for j in range(BINS):
            rows = pl.ds((1 + i) * 8 + j, regions, stride=8 * SLOTS)
            lhs[i % 2, :, j * channels:j * channels + half] = acc_a[rows, :].astype(jnp.bfloat16)
            lhs[i % 2, :, j * channels + half:(j + 1) * channels] = acc_b[rows, :].astype(jnp.bfloat16)
        weights(i).wait()
        part = jnp.dot(lhs[i % 2], wbuf[i % depth], preferred_element_type=jnp.float32)
        if i == 0:
            out_ref[...] = part
        else:
            out_ref[...] += part
        if i + depth < BINS:
            weights(i + depth).start()


def pool_and_project(group, codes, plan, total, joins, tab, own, mate, halo, w_one):
    tile_rows, feat_w, channels = own.shape
    regions = tab.shape[0]
    hidden = w_one.shape[1]
    row_in = BINS * channels
    depth = 3
    dims = (group, tile_rows, feat_w, channels, regions)
    smem = pl.BlockSpec(memory_space=pltpu.SMEM)
    vmem = pl.BlockSpec(memory_space=pltpu.VMEM)
    hbm = pl.BlockSpec(memory_space=pl.ANY)
    return pl.pallas_call(
        functools.partial(pool_kernel, dims),
        out_shape=jax.ShapeDtypeStruct((regions, hidden), jnp.float32),
        in_specs=[smem] * 4 + [vmem] + [hbm] * 4,
        out_specs=vmem,
        scratch_shapes=[
            pltpu.VMEM((2 * tile_rows + HALO, feat_w, channels), jnp.bfloat16),
            pltpu.VMEM((regions * SLOTS * 8, channels // 2), jnp.float32),
            pltpu.VMEM((regions * SLOTS * 8, channels // 2), jnp.float32),
            pltpu.VMEM((2, regions, row_in), jnp.bfloat16),
            pltpu.VMEM((depth, row_in, hidden), jnp.bfloat16),
            pltpu.VMEM((2, BLOCK * 8, channels), jnp.float32),
            pltpu.VMEM((2, BLOCK * 8, channels), jnp.float32),
            pltpu.SemaphoreType.DMA((3,)),
            pltpu.SemaphoreType.DMA((depth,)),
        ],
        compiler_params=pltpu.CompilerParams(vmem_limit_bytes=64 * 1024 * 1024 - 65536),
        cost_estimate=pl.CostEstimate(flops=30_000_000_000, bytes_accessed=50_000_000, transcendentals=0),
        name='pool',
    )(codes, plan, total, joins, tab, own, mate, halo, w_one)


def solution(mesh):
    group = mesh.shape['sp']

    def device_step(feature_map, box_coords, w_one, b_one, w_two, b_two):
        tile_rows, feat_w, channels = feature_map.shape
        regions = box_coords.shape[0] // group
        me = lax.axis_index('sp')
        chip, core = me // 2, me % 2

        mate = lax.ppermute(feature_map, 'sp', [(0, 1), (1, 0), (2, 3), (3, 2)])
        rim = jnp.where(core == 1, feature_map[tile_rows - HALO:], feature_map[:HALO])
        hop_one = lax.ppermute(rim, 'sp', [(1, 2), (2, 1)])
        hop_two = lax.ppermute(hop_one, 'sp', [(1, 0), (2, 3)])
        halo = jnp.where((me == 1) | (me == 2), hop_one, hop_two)

        far = (me + 2) % 4
        boxes = jnp.stack([lax.dynamic_slice_in_dim(box_coords, g * regions, regions, 0) for g in (far, me)])
        tab, right = column_table(boxes, feat_w)
        codes, plan, total, joins = row_lists(boxes, right, chip, tile_rows, tile_rows * group)

        def project(g):
            return pool_and_project(g, codes, plan, total, joins, tab[g], feature_map, mate, halo, w_one)

        away = project(0)
        back = lax.ppermute(away, 'sp', [(0, 2), (2, 0), (1, 3), (3, 1)])
        here = project(1)
        hidden_act = jnp.maximum(here + back + b_one, 0.0).astype(jnp.bfloat16)
        return jnp.maximum(jnp.dot(hidden_act, w_two, preferred_element_type=jnp.float32) + b_two, 0.0).astype(jnp.bfloat16)

    return jax.shard_map(device_step, mesh=mesh, in_specs=(P(('dp', 'sp'), None, None), P('dp', None), P(), P(), P(), P()), out_specs=P(('dp', 'sp'), None), check_vma=False)
```

```python
import functools

import jax
import jax.numpy as jnp
from jax import lax
from jax.experimental import pallas as pl
from jax.experimental.pallas import tpu as pltpu
from jax.sharding import PartitionSpec as P

BINS = 7
SAMPLES = 2 * BINS
HALO = 6
WINDOW = 256
BLOCK = 16
GAINS = 33
TURNS = 4
PIECES = 4
SLOTS = 11


def sample_rows(start_eighths, span_units, length):
    ids = jnp.arange(SAMPLES, dtype=jnp.int32)
    pos = 4 * start_eighths[..., None] - 16 + (2 * ids + 1) * span_units[..., None]
    inside = (pos >= -32) & (pos <= 32 * length)
    return pos, inside


def column_table(boxes, feat_w):
    pos, inside = sample_rows(boxes[..., 1], (boxes[..., 3] - boxes[..., 1]) // 7, feat_w)
    pos = jnp.clip(pos, 0, 32 * (feat_w - 1))
    right = pos[..., 0] // 32 >= feat_w - WINDOW
    shift = jnp.where(right, feat_w - WINDOW, 0)
    at = (pos - 32 * shift[..., None]).astype(jnp.float32) / 32.0
    gain = jnp.where(inside, 0.5, 0.0)
    pad = [(0, 0)] * (at.ndim - 1) + [(0, 1)]
    cols = lax.broadcasted_iota(jnp.float32, at.shape[:-1] + (BINS + 1, WINDOW), at.ndim)

    def tent(which):
        x = jnp.pad(at[..., which::2], pad)[..., None]
        g = jnp.pad(gain[..., which::2], pad)[..., None]
        return jnp.maximum(1.0 - jnp.abs(cols - x), 0.0) * g

    return tent(0) + tent(1), right


def row_lists(boxes, right, chip, tile_rows, length):
    regions = boxes.shape[-2]
    chip_rows = 2 * tile_rows
    lists, codes, plans = list_sizes(regions, tile_rows)
    pos, inside = sample_rows(boxes[..., 0], (boxes[..., 2] - boxes[..., 0]) // 7, length)
    pos = jnp.maximum(pos, 0)
    at_top = pos // 32 >= length - 1
    low = jnp.where(at_top, length - 2, pos // 32)
    frac = jnp.where(at_top, 32, pos % 32)
    first, last = low[..., 0::2], low[..., 1::2] + 1
    owned = (first + last) // 2 // chip_rows == chip
    tile = first // tile_rows
    straddle = owned & (last // tile_rows > tile)

    def per_sample(a):
        return jnp.repeat(a, 2, axis=-1)

    edge = per_sample((tile + 1) * tile_rows)
    part_slot = 1 + BINS + per_sample(tile % 2)
    upper = per_sample(straddle) & (low >= edge)
    split = per_sample(straddle) & (low == edge - 1)
    start = chip * (chip_rows - HALO)
    side = right[..., None].astype(jnp.int32)
    live = per_sample(owned) & inside
    slot = jnp.where(upper, part_slot, 1 + jnp.arange(SAMPLES, dtype=jnp.int32) // 2)
    ids = jnp.arange(regions, dtype=jnp.int32)[:, None]
    gain = frac + jnp.where(split, GAINS, 0)
    keys = gain + (slot << 7) + (ids << 11) + ((2 * jnp.where(live, low - start, lists) + side) << 19)
    extra = []
    for q in range(2):
        here = split & live & per_sample(tile % 2 == q)
        number = lists - 2 + (q - chip) % 2
        key = jnp.max(jnp.where(here, frac + 2 * GAINS + ((1 + BINS + q) << 7) + (ids << 11) + ((2 * number + side) << 19), -1), axis=-1)
        extra.append(jnp.where(key < 0, (2 * lists) << 19, key))
    keys = jnp.concatenate([keys, jnp.stack(extra, axis=-1)], axis=-1)
    keys = jnp.sort(keys.reshape(keys.shape[0], -1), axis=-1)
    region = (keys >> 11) & 255
    code = (region * SLOTS + ((keys >> 7) & 15)) * 8 + ((keys & 127) << 15) + (region << 22)
    code = jnp.pad(code, ((0, 0), (0, codes - code.shape[-1])))

    order = jnp.arange(2 * lists + 1, dtype=jnp.int32)
    ahead = jnp.sum((keys[:, None, :] < (order << 19)[:, None]).astype(jnp.int32), axis=-1)
    begin, count = ahead[:, :-1], ahead[:, 1:] - ahead[:, :-1]
    blocks = (count + BLOCK - 1) // BLOCK
    order = order[:-1]
    prior = jnp.sum(jnp.where(order[:, None] < order[None, :], blocks[:, :, None], 0), axis=1)
    turn = jnp.arange(plans, dtype=jnp.int32)[:, None] - 1
    nth = turn - prior[:, None, :]
    packed = order + (jnp.minimum(count[:, None, :] - BLOCK * nth, BLOCK) << 8) + ((begin[:, None, :] + BLOCK * nth) << 13)
    plan = jnp.sum(jnp.where((nth >= 0) & (nth < blocks[:, None, :]), packed, 0), axis=-1)
    reach = chip * HALO + tile_rows // 2 * jnp.arange(1, PIECES, dtype=jnp.int32) - 1
    bounds = [jnp.sum(jnp.where(order < 2 * reach[:, None], blocks[:, None, :], 0), axis=-1), jnp.sum(blocks, axis=-1, keepdims=True)]
    bounds = jnp.concatenate(bounds, axis=-1)

    bins = jnp.arange(BINS, dtype=jnp.int32) + 1
    joins = jnp.stack([jnp.sum(jnp.where(straddle & (tile % 2 == q), bins, 0), axis=-1) for q in range(2)], axis=-1)
    return code.reshape(-1), plan.reshape(-1), bounds.reshape(-1), joins.reshape(-1)


def list_sizes(regions, tile_rows):
    lists = 2 * tile_rows + HALO - 1 + 2
    codes = regions * (SAMPLES + 2) + BLOCK
    plans = (regions * (SAMPLES + 2) + (BLOCK - 1) * 2 * lists) // BLOCK + 8
    return lists, codes, plans


def pool_kernel(dims, code_ref, plan_ref, bound_ref, join_ref, tab_ref, own_ref, mate_ref, halo_ref, w_ref, out_ref,
                feat, acc_a, acc_b, gain, lhs, wbuf, out_one, out_two, fsem, hsem, wsem):
    group, tile_rows, feat_w, channels, regions = dims
    lists, codes, plans = list_sizes(regions, tile_rows)
    me = lax.axis_index('sp')
    chip, core = me // 2, me % 2
    edge_one = tile_rows - 1 + chip * (tile_rows - 2 * tile_rows + HALO)
    edge_two = edge_one + tile_rows
    half = channels // 2
    row_in = BINS * channels
    first = chip * HALO
    some = tile_rows // 2

    def piece(source, q, part):
        return pltpu.make_async_copy(source.at[pl.ds(part * some, some)], feat.at[pl.ds(first + q * some, some)], fsem.at[q])

    edge = pltpu.make_async_copy(halo_ref, feat.at[pl.ds((1 - chip) * 2 * tile_rows, HALO)], hsem)
    edge.start()

    @pl.when(core == 0)
    def _():
        for q, (source, part) in enumerate([(own_ref, 0), (own_ref, 1), (mate_ref, 0), (mate_ref, 1)]):
            piece(source, q, part).start()

    @pl.when(core == 1)
    def _():
        for q, (source, part) in enumerate([(mate_ref, 0), (mate_ref, 1), (own_ref, 0), (own_ref, 1)]):
            piece(source, q, part).start()

    depth = wbuf.shape[0]

    def weights(i):
        return pltpu.make_async_copy(w_ref.at[pl.ds(i * row_in, row_in)], wbuf.at[i % depth], wsem.at[i % depth])

    zero = jnp.zeros((8 * SLOTS, half), jnp.float32)

    def clear(r, _):
        at = pl.ds(pl.multiple_of(r * 8 * SLOTS, 8), 8 * SLOTS)
        acc_a[at, :] = zero
        acc_b[at, :] = zero
        return 0

    lax.fori_loop(0, regions, clear, 0)

    def fill(f, _):
        high = jnp.full((8, half), f, jnp.int32).astype(jnp.float32) / 64.0
        for kind in range(3):
            at = pl.multiple_of((f + kind * GAINS) * 16, 16)
            gain[pl.ds(at, 8), :] = jnp.zeros_like(high) if kind == 2 else 0.5 - high
            gain[pl.ds(at + 8, 8), :] = jnp.zeros_like(high) if kind == 1 else high
        return 0

    lax.fori_loop(0, GAINS, fill, 0)

    def multiply(turn, out):
        plan = plan_ref[group * plans + turn]
        v = (plan & 255) >> 1
        column = pl.multiple_of((plan & 1) * (feat_w - WINDOW), 16)
        at = group * codes + (plan >> 13)
        rows = [tab_ref[code_ref[at + s] >> 22] for s in range(BLOCK)]
        left = jnp.concatenate(rows, axis=0).astype(jnp.bfloat16)
        row = jnp.where(v < lists - 2, v, jnp.where(v == lists - 2, edge_one, edge_two))
        out[0] = jnp.dot(left, feat[row, pl.ds(column, WINDOW), :], preferred_element_type=jnp.float32)
        out[1] = jnp.dot(left, feat[row + 1, pl.ds(column, WINDOW), :], preferred_element_type=jnp.float32)

    def spread(turn, out):
        plan = plan_ref[group * plans + turn]
        live = (plan >> 8) & 31
        at = group * codes + (plan >> 13)
        for s0 in range(0, BLOCK, 4):
            slots, news = [], []
            for s in range(s0, s0 + 4):
                code = jnp.where(s < live, code_ref[at + s], 0)
                weight = pl.multiple_of((code >> 11) & (127 << 4), 16)
                wl, wh = gain[pl.ds(weight, 8), :], gain[pl.ds(weight + 8, 8), :]
                slot = pl.ds(pl.multiple_of(code & 32767, 8), 8)
                slots.append(slot)
                news.append((
                    acc_a[slot, :] + (out[0, 8 * s:8 * s + 8, :half] * wl + out[1, 8 * s:8 * s + 8, :half] * wh),
                    acc_b[slot, :] + (out[0, 8 * s:8 * s + 8, half:] * wl + out[1, 8 * s:8 * s + 8, half:] * wh),
                ))
            for slot, (a, b) in zip(slots, news):
                acc_a[slot, :] = a
                acc_b[slot, :] = b

    def turns(u, _):
        for t in range(0, TURNS, 2):
            multiply(TURNS * u + t + 1, out_one)
            spread(TURNS * u + t, out_two)
            multiply(TURNS * u + t + 2, out_two)
            spread(TURNS * u + t + 1, out_one)
        return 0

    out_two[...] = jnp.zeros_like(out_two)
    edge.wait()

    def phase(q, done):
        piece(own_ref, q, 0).wait()

        @pl.when(q == PIECES - 1)
        def _():
            for i in range(depth):
                weights(i).start()

        bound = bound_ref[group * PIECES + q]
        upto = jnp.where(q == PIECES - 1, (bound + TURNS - 1) // TURNS, bound // TURNS)
        lax.fori_loop(done, upto, turns, 0)
        return upto

    done = lax.fori_loop(0, PIECES, phase, 0)
    spread(TURNS * done, out_two)

    def join(r4, _):
        news = []
        for r in range(4):
            for q in range(2):
                row = r4 * 4 + r
                to = pl.ds(pl.multiple_of((row * SLOTS + join_ref[(group * regions + row) * 2 + q]) * 8, 8), 8)
                part = pl.ds(pl.multiple_of((row * SLOTS + 1 + BINS + q) * 8, 8), 8)
                for acc in (acc_a, acc_b):
                    news.append((acc, to, acc[to, :].astype(jnp.bfloat16).astype(jnp.float32) + acc[part, :].astype(jnp.bfloat16).astype(jnp.float32)))
        for acc, to, value in news:
            acc[to, :] = value
        return 0

    lax.fori_loop(0, regions // 4, join, 0)

    for i in range(BINS):
        for j in range(BINS):
            rows = pl.ds((1 + i) * 8 + j, regions, stride=8 * SLOTS)
            lhs[i % 2, :, j * channels:j * channels + half] = acc_a[rows, :].astype(jnp.bfloat16)
            lhs[i % 2, :, j * channels + half:(j + 1) * channels] = acc_b[rows, :].astype(jnp.bfloat16)
        weights(i).wait()
        part = jnp.dot(lhs[i % 2], wbuf[i % depth], preferred_element_type=jnp.float32)
        if i == 0:
            out_ref[...] = part
        else:
            out_ref[...] += part
        if i + depth < BINS:
            weights(i + depth).start()


def pool_and_project(group, codes, plan, bounds, joins, tab, own, mate, halo, w_one):
    tile_rows, feat_w, channels = own.shape
    regions = tab.shape[0]
    hidden = w_one.shape[1]
    row_in = BINS * channels
    depth = 3
    dims = (group, tile_rows, feat_w, channels, regions)
    smem = pl.BlockSpec(memory_space=pltpu.SMEM)
    vmem = pl.BlockSpec(memory_space=pltpu.VMEM)
    hbm = pl.BlockSpec(memory_space=pl.ANY)
    return pl.pallas_call(
        functools.partial(pool_kernel, dims),
        out_shape=jax.ShapeDtypeStruct((regions, hidden), jnp.float32),
        in_specs=[smem] * 4 + [vmem] + [hbm] * 4,
        out_specs=vmem,
        scratch_shapes=[
            pltpu.VMEM((2 * tile_rows + HALO, feat_w, channels), jnp.bfloat16),
            pltpu.VMEM((regions * SLOTS * 8, channels // 2), jnp.float32),
            pltpu.VMEM((regions * SLOTS * 8, channels // 2), jnp.float32),
            pltpu.VMEM((3 * GAINS * 16, channels // 2), jnp.float32),
            pltpu.VMEM((2, regions, row_in), jnp.bfloat16),
            pltpu.VMEM((depth, row_in, hidden), jnp.bfloat16),
            pltpu.VMEM((2, BLOCK * 8, channels), jnp.float32),
            pltpu.VMEM((2, BLOCK * 8, channels), jnp.float32),
            pltpu.SemaphoreType.DMA((PIECES,)),
            pltpu.SemaphoreType.DMA(()),
            pltpu.SemaphoreType.DMA((depth,)),
        ],
        compiler_params=pltpu.CompilerParams(vmem_limit_bytes=64 * 1024 * 1024 - 65536),
        cost_estimate=pl.CostEstimate(flops=30_000_000_000, bytes_accessed=50_000_000, transcendentals=0),
        name='pool',
    )(codes, plan, bounds, joins, tab, own, mate, halo, w_one)


def solution(mesh):
    group = mesh.shape['sp']

    def device_step(feature_map, box_coords, w_one, b_one, w_two, b_two):
        tile_rows, feat_w, channels = feature_map.shape
        regions = box_coords.shape[0] // group
        me = lax.axis_index('sp')
        chip, core = me // 2, me % 2

        mate = lax.ppermute(feature_map, 'sp', [(0, 1), (1, 0), (2, 3), (3, 2)])
        rim = jnp.where(core == 1, feature_map[tile_rows - HALO:], feature_map[:HALO])
        hop_one = lax.ppermute(rim, 'sp', [(1, 2), (2, 1)])
        hop_two = lax.ppermute(hop_one, 'sp', [(1, 0), (2, 3)])
        halo = jnp.where((me == 1) | (me == 2), hop_one, hop_two)

        far = (me + 2) % 4
        boxes = jnp.stack([lax.dynamic_slice_in_dim(box_coords, g * regions, regions, 0) for g in (far, me)])
        tab, right = column_table(boxes, feat_w)
        codes, plan, bounds, joins = row_lists(boxes, right, chip, tile_rows, tile_rows * group)

        def project(g):
            return pool_and_project(g, codes, plan, bounds, joins, tab[g], feature_map, mate, halo, w_one)

        away = project(0)
        back = lax.ppermute(away, 'sp', [(0, 2), (2, 0), (1, 3), (3, 1)])
        here = project(1)
        hidden_act = jnp.maximum(here + back + b_one, 0.0).astype(jnp.bfloat16)
        return jnp.maximum(jnp.dot(hidden_act, w_two, preferred_element_type=jnp.float32) + b_two, 0.0).astype(jnp.bfloat16)

    return jax.shard_map(device_step, mesh=mesh, in_specs=(P(('dp', 'sp'), None, None), P('dp', None), P(), P(), P(), P()), out_specs=P(('dp', 'sp'), None), check_vma=False)
```

```python
import functools

import jax
import jax.numpy as jnp
from jax import lax
from jax.experimental import pallas as pl
from jax.experimental.pallas import tpu as pltpu
from jax.sharding import PartitionSpec as P

BINS = 7
SAMPLES = 2 * BINS
HALO = 6
WINDOW = 256
BLOCK = 16
GAINS = 33
TURNS = 4
PIECES = 4
SLOTS = 10
PITCH = SLOTS * 16 + 24


def sample_rows(start_eighths, span_units, length):
    ids = jnp.arange(SAMPLES, dtype=jnp.int32)
    pos = 4 * start_eighths[..., None] - 16 + (2 * ids + 1) * span_units[..., None]
    inside = (pos >= -32) & (pos <= 32 * length)
    return pos, inside


def column_table(boxes, feat_w):
    pos, inside = sample_rows(boxes[..., 1], (boxes[..., 3] - boxes[..., 1]) // 7, feat_w)
    pos = jnp.clip(pos, 0, 32 * (feat_w - 1))
    right = pos[..., 0] // 32 >= feat_w - WINDOW
    shift = jnp.where(right, feat_w - WINDOW, 0)
    at = (pos - 32 * shift[..., None]).astype(jnp.float32) / 32.0
    gain = jnp.where(inside, 0.5, 0.0)
    pad = [(0, 0)] * (at.ndim - 1) + [(0, 1)]
    cols = lax.broadcasted_iota(jnp.float32, at.shape[:-1] + (BINS + 1, WINDOW), at.ndim)

    def tent(which):
        x = jnp.pad(at[..., which::2], pad)[..., None]
        g = jnp.pad(gain[..., which::2], pad)[..., None]
        return jnp.maximum(1.0 - jnp.abs(cols - x), 0.0) * g

    return tent(0) + tent(1), right


def row_lists(boxes, right, chip, tile_rows, length):
    regions = boxes.shape[-2]
    chip_rows = 2 * tile_rows
    lists, plans = list_sizes(regions, tile_rows)
    pos, inside = sample_rows(boxes[..., 0], (boxes[..., 2] - boxes[..., 0]) // 7, length)
    pos = jnp.maximum(pos, 0)
    at_top = pos // 32 >= length - 1
    low = jnp.where(at_top, length - 2, pos // 32)
    frac = jnp.where(at_top, 32, pos % 32)
    first, last = low[..., 0::2], low[..., 1::2] + 1
    owned = (first + last) // 2 // chip_rows == chip
    tile = first // tile_rows
    straddle = owned & (last // tile_rows > tile)

    def per_sample(a):
        return jnp.repeat(a, 2, axis=-1)

    edge = per_sample((tile + 1) * tile_rows)
    part_slot = 1 + BINS + per_sample(tile % 2)
    upper = per_sample(straddle) & (low >= edge)
    split = per_sample(straddle) & (low == edge - 1)
    start = chip * (chip_rows - HALO)
    side = right[..., None].astype(jnp.int32)
    live = per_sample(owned) & inside
    slot = jnp.where(upper, part_slot, 1 + jnp.arange(SAMPLES, dtype=jnp.int32) // 2)
    ids = jnp.arange(regions, dtype=jnp.int32)[:, None]
    gain = frac + jnp.where(split, GAINS, 0)
    keys = gain + (slot << 7) + (ids << 11) + ((2 * jnp.where(live, low - start, lists) + side) << 19)
    extra = []
    for q in range(2):
        here = split & live & per_sample(tile % 2 == q)
        number = lists - 2 + (q - chip) % 2
        key = jnp.max(jnp.where(here, frac + 2 * GAINS + ((1 + BINS + q) << 7) + (ids << 11) + ((2 * number + side) << 19), -1), axis=-1)
        extra.append(jnp.where(key < 0, (2 * lists) << 19, key))
    keys = jnp.concatenate([keys, jnp.stack(extra, axis=-1)], axis=-1)
    groups, per = keys.shape[0], regions * (SAMPLES + 2)
    number = keys >> 19
    ids = jnp.arange(16, dtype=jnp.int32)
    coarse = ((number >> 4)[..., None] == ids).astype(jnp.bfloat16)
    fine = ((number & 15)[..., None] == ids).astype(jnp.bfloat16)
    count = jnp.einsum('grka,grkb->gab', coarse, fine, preferred_element_type=jnp.float32).astype(jnp.int32).reshape(groups, 256)
    order = jnp.arange(256, dtype=jnp.int32)
    count = jnp.where(order < 2 * lists, count, 0)

    keys = jnp.sort((keys + (jnp.arange(groups, dtype=jnp.int32) << 27)[:, None, None]).reshape(-1))
    keys = jnp.pad(keys, (0, BLOCK))
    region = (keys >> 11) & 255
    slots = region * PITCH + ((keys >> 7) & 15) * 16
    gains = (keys & 127) << 4

    blocks = (count + BLOCK - 1) // BLOCK
    earlier = order[:, None] < order[None, :]
    begin = jnp.sum(jnp.where(earlier, count[:, :, None], 0), axis=1) + per * jnp.arange(groups, dtype=jnp.int32)[:, None]
    prior = jnp.sum(jnp.where(earlier, blocks[:, :, None], 0), axis=1)
    turn = jnp.arange(groups * plans, dtype=jnp.int32)[:, None]

    def of(a):
        return jnp.where(turn < plans, a[0], a[1])

    turn_in = turn % plans
    nth = turn_in - 1 - of(prior)
    packed = order + (jnp.minimum(of(count) - BLOCK * nth, BLOCK) << 8) + ((of(begin) + BLOCK * nth) << 13)
    piece = turn_in - (plans - PIECES)
    reach = jnp.where(piece == PIECES - 1, 2 * lists, 2 * (chip * HALO + tile_rows // 2 * (piece + 1) - 1))
    chosen = jnp.where(piece < 0, jnp.where((nth >= 0) & (nth < of(blocks)), packed, 0), jnp.where(order < reach, of(blocks), 0))
    plan = jnp.sum(chosen, axis=-1)

    bins = jnp.arange(BINS, dtype=jnp.int32) + 1
    joins = jnp.concatenate([jnp.sum(jnp.where(straddle & (tile % 2 == q), bins, 0), axis=-1) for q in range(2)], axis=0)
    return slots, gains, region, plan, joins


def list_sizes(regions, tile_rows):
    lists = 2 * tile_rows + HALO - 1 + 2
    plans = (regions * (SAMPLES + 2) + (BLOCK - 1) * 2 * lists) // BLOCK + TURNS + 4 + PIECES
    return lists, plans


def pool_kernel(dims, slot_ref, gain_ref, tab_at_ref, plan_ref, join_ref, tabs_ref, own_ref, mate_ref, halo_ref, relay_ref, w_ref, out_ref,
                feat, tab_ref, acc, gain, lhs, wbuf, out_one, out_two, fsem, hsem, tsem, wsem):
    group, tile_rows, feat_w, channels, regions = dims
    lists, plans = list_sizes(regions, tile_rows)
    me = lax.axis_index('sp')
    chip, core = me // 2, me % 2
    edge_one = tile_rows - 1 + chip * (tile_rows - 2 * tile_rows + HALO)
    edge_two = edge_one + tile_rows
    half = channels // 2
    row_in = BINS * channels
    first = chip * HALO
    some = tile_rows // 2

    def piece(source, q, part):
        return pltpu.make_async_copy(source.at[pl.ds(part * some, some)], feat.at[pl.ds(first + q * some, some)], fsem.at[q])

    def edge(source):
        return pltpu.make_async_copy(source, feat.at[pl.ds((1 - chip) * 2 * tile_rows, HALO)], hsem)

    columns = pltpu.make_async_copy(tabs_ref.at[group], tab_ref, tsem)
    columns.start()

    @pl.when(chip != core)
    def _():
        edge(halo_ref).start()

    @pl.when(chip == core)
    def _():
        edge(relay_ref).start()

    @pl.when(core == 0)
    def _():
        for q, (source, part) in enumerate([(own_ref, 0), (own_ref, 1), (mate_ref, 0), (mate_ref, 1)]):
            piece(source, q, part).start()

    @pl.when(core == 1)
    def _():
        for q, (source, part) in enumerate([(mate_ref, 0), (mate_ref, 1), (own_ref, 0), (own_ref, 1)]):
            piece(source, q, part).start()

    depth = wbuf.shape[0]

    def weights(i):
        return pltpu.make_async_copy(w_ref.at[pl.ds(i * row_in, row_in)], wbuf.at[i % depth], wsem.at[i % depth])

    zero = jnp.zeros((16 * SLOTS, half), jnp.float32)

    def clear(r, _):
        acc[pl.ds(pl.multiple_of(r * PITCH, 8), 16 * SLOTS), :] = zero
        return 0

    lax.fori_loop(0, regions, clear, 0)

    def fill(f, _):
        high = jnp.full((8, half), f, jnp.int32).astype(jnp.float32) / 64.0
        for kind in range(3):
            at = pl.multiple_of((f + kind * GAINS) * 16, 16)
            gain[pl.ds(at, 8), :] = jnp.zeros_like(high) if kind == 2 else 0.5 - high
            gain[pl.ds(at + 8, 8), :] = jnp.zeros_like(high) if kind == 1 else high
        return 0

    lax.fori_loop(0, GAINS, fill, 0)

    def multiply(turn, out):
        plan = plan_ref[group * plans + turn]
        v = (plan & 255) >> 1
        column = pl.multiple_of((plan & 1) * (feat_w - WINDOW), 16)
        at = plan >> 13
        left = jnp.concatenate([tab_ref[tab_at_ref[at + s]] for s in range(BLOCK)], axis=0).astype(jnp.bfloat16)
        row = jnp.where(v < lists - 2, v, jnp.where(v == lists - 2, edge_one, edge_two))
        out[0] = jnp.dot(left, feat[row, pl.ds(column, WINDOW), :], preferred_element_type=jnp.float32)
        out[1] = jnp.dot(left, feat[row + 1, pl.ds(column, WINDOW), :], preferred_element_type=jnp.float32)

    def spread(turn, out):
        plan = plan_ref[group * plans + turn]
        live = (plan >> 8) & 31
        at = plan >> 13
        for s0 in range(0, BLOCK, 4):
            news = []
            for s in range(s0, s0 + 4):
                slot = pl.multiple_of(jnp.where(s < live, slot_ref[at + s], 0), 8)
                weight = pl.multiple_of(gain_ref[at + s], 16)
                wl, wh = gain[pl.ds(weight, 8), :], gain[pl.ds(weight + 8, 8), :]
                for c in range(2):
                    to = pl.ds(slot + 8 * c, 8)
                    cols = slice(c * half, (c + 1) * half)
                    news.append((to, acc[to, :] + (out[0, 8 * s:8 * s + 8, cols] * wl + out[1, 8 * s:8 * s + 8, cols] * wh)))
            for to, value in news:
                acc[to, :] = value

    def turns(u, _):
        for t in range(0, TURNS, 2):
            multiply(TURNS * u + t + 1, out_one)
            spread(TURNS * u + t, out_two)
            multiply(TURNS * u + t + 2, out_two)
            spread(TURNS * u + t + 1, out_one)
        return 0

    out_two[...] = jnp.zeros_like(out_two)
    columns.wait()
    edge(halo_ref).wait()

    def phase(q, done):
        piece(own_ref, q, 0).wait()

        @pl.when(q == PIECES - 1)
        def _():
            for i in range(depth):
                weights(i).start()

        bound = plan_ref[(group + 1) * plans - PIECES + q]
        upto = jnp.where(q == PIECES - 1, (bound + TURNS - 1) // TURNS, bound // TURNS)
        lax.fori_loop(done, upto, turns, 0)
        return upto

    done = lax.fori_loop(0, PIECES, phase, 0)
    spread(TURNS * done, out_two)

    def join(r4, _):
        news = []
        for r in range(4):
            for q in range(2):
                row = r4 * 4 + r
                base = row * PITCH
                for c in range(2):
                    to = pl.ds(pl.multiple_of(base + join_ref[2 * q + group, row] * 16 + 8 * c, 8), 8)
                    part = pl.ds(pl.multiple_of(base + (1 + BINS + q) * 16 + 8 * c, 8), 8)
                    news.append((to, acc[to, :].astype(jnp.bfloat16).astype(jnp.float32) + acc[part, :].astype(jnp.bfloat16).astype(jnp.float32)))
        for to, value in news:
            acc[to, :] = value
        return 0

    lax.fori_loop(0, regions // 4, join, 0)

    for i in range(BINS):
        for j in range(BINS):
            for c in range(2):
                rows = pl.ds((1 + i) * 16 + 8 * c + j, regions, stride=PITCH)
                lhs[i % 2, :, j * channels + c * half:j * channels + (c + 1) * half] = acc[rows, :].astype(jnp.bfloat16)
        weights(i).wait()
        part = jnp.dot(lhs[i % 2], wbuf[i % depth], preferred_element_type=jnp.float32)
        if i == 0:
            out_ref[...] = part
        else:
            out_ref[...] += part
        if i + depth < BINS:
            weights(i + depth).start()


def pool_and_project(group, slots, gains, tab_at, plan, joins, tab, own, mate, halo, relay, w_one):
    tile_rows, feat_w, channels = own.shape
    regions = tab.shape[1]
    hidden = w_one.shape[1]
    row_in = BINS * channels
    depth = 3
    dims = (group, tile_rows, feat_w, channels, regions)
    smem = pl.BlockSpec(memory_space=pltpu.SMEM)
    vmem = pl.BlockSpec(memory_space=pltpu.VMEM)
    hbm = pl.BlockSpec(memory_space=pl.ANY)
    return pl.pallas_call(
        functools.partial(pool_kernel, dims),
        out_shape=jax.ShapeDtypeStruct((regions, hidden), jnp.float32),
        in_specs=[smem] * 5 + [hbm] * 6,
        out_specs=vmem,
        scratch_shapes=[
            pltpu.VMEM((2 * tile_rows + HALO, feat_w, channels), jnp.bfloat16),
            pltpu.VMEM(tab.shape[1:], jnp.float32),
            pltpu.VMEM((regions * PITCH, channels // 2), jnp.float32),
            pltpu.VMEM((3 * GAINS * 16, channels // 2), jnp.float32),
            pltpu.VMEM((2, regions, row_in), jnp.bfloat16),
            pltpu.VMEM((depth, row_in, hidden), jnp.bfloat16),
            pltpu.VMEM((2, BLOCK * 8, channels), jnp.float32),
            pltpu.VMEM((2, BLOCK * 8, channels), jnp.float32),
            pltpu.SemaphoreType.DMA((PIECES,)),
            pltpu.SemaphoreType.DMA(()),
            pltpu.SemaphoreType.DMA(()),
            pltpu.SemaphoreType.DMA((depth,)),
        ],
        compiler_params=pltpu.CompilerParams(vmem_limit_bytes=64 * 1024 * 1024 - 65536),
        cost_estimate=pl.CostEstimate(flops=30_000_000_000, bytes_accessed=50_000_000, transcendentals=0),
        name='pool',
    )(slots, gains, tab_at, plan, joins, tab, own, mate, halo, relay, w_one)


def solution(mesh):
    group = mesh.shape['sp']

    def device_step(feature_map, box_coords, w_one, b_one, w_two, b_two):
        tile_rows, feat_w, channels = feature_map.shape
        regions = box_coords.shape[0] // group
        me = lax.axis_index('sp')
        chip, core = me // 2, me % 2

        mate = lax.ppermute(feature_map, 'sp', [(0, 1), (1, 0), (2, 3), (3, 2)])
        rim = jnp.where(core == 1, feature_map[tile_rows - HALO:], feature_map[:HALO])
        hop_one = lax.ppermute(rim, 'sp', [(1, 2), (2, 1)])
        hop_two = lax.ppermute(hop_one, 'sp', [(1, 0), (2, 3)])

        far = (me + 2) % 4
        boxes = jnp.stack([lax.dynamic_slice_in_dim(box_coords, g * regions, regions, 0) for g in (far, me)])
        tab, right = column_table(boxes, feat_w)
        lists = row_lists(boxes, right, chip, tile_rows, tile_rows * group)

        def project(g):
            return pool_and_project(g, *lists, tab, feature_map, mate, hop_one, hop_two, w_one)

        away = project(0)
        back = lax.ppermute(away, 'sp', [(0, 2), (2, 0), (1, 3), (3, 1)])
        here = project(1)
        hidden_act = jnp.maximum(here + back + b_one, 0.0).astype(jnp.bfloat16)
        return jnp.maximum(jnp.dot(hidden_act, w_two, preferred_element_type=jnp.float32) + b_two, 0.0).astype(jnp.bfloat16)

    return jax.shard_map(device_step, mesh=mesh, in_specs=(P(('dp', 'sp'), None, None), P('dp', None), P(), P(), P(), P()), out_specs=P(('dp', 'sp'), None), check_vma=False)
```

```python
import functools

import jax
import jax.numpy as jnp
from jax import lax
from jax.experimental import pallas as pl
from jax.experimental.pallas import tpu as pltpu
from jax.sharding import PartitionSpec as P

BINS = 7
SAMPLES = 2 * BINS
HALO = 6
WINDOW = 256
BLOCK = 16
GAINS = 33
SPILL = 1024
TURNS = 12
PIECES = 4
SLOTS = 10
SPARE = 4


def sample_rows(start_eighths, span_units, length):
    ids = jnp.arange(SAMPLES, dtype=jnp.int32)
    pos = 4 * start_eighths[..., None] - 16 + (2 * ids + 1) * span_units[..., None]
    inside = (pos >= -32) & (pos <= 32 * length)
    return pos, inside


def column_table(boxes, feat_w):
    start, span = boxes[..., 1, None], (boxes[..., 3, None] - boxes[..., 1, None]) // 7
    right = jnp.maximum(4 * start - 16 + span, 0) // 32 >= feat_w - WINDOW
    shift = jnp.where(right, feat_w - WINDOW, 0)
    ids = jnp.arange(BINS + 1, dtype=jnp.int32)
    cols = lax.broadcasted_iota(jnp.float32, start.shape[:-1] + (BINS + 1, WINDOW), start.ndim)

    def tent(which):
        pos = 4 * start - 16 + (4 * ids + 2 * which + 1) * span
        inside = (pos >= -32) & (pos <= 32 * feat_w) & (ids < BINS)
        at = (jnp.clip(pos, 0, 32 * (feat_w - 1)) - 32 * shift).astype(jnp.float32) / 32.0
        return jnp.maximum(1.0 - jnp.abs(cols - jnp.where(inside, at, -4.0)[..., None]), 0.0)

    return (tent(0) + tent(1)) * 0.5, right[..., 0]


def row_lists(boxes, right, chip, tile_rows, length):
    regions = boxes.shape[-2]
    chip_rows = 2 * tile_rows
    lists, plans = list_sizes(regions, tile_rows)
    pos, inside = sample_rows(boxes[..., 0], (boxes[..., 2] - boxes[..., 0]) // 7, length)
    pos = jnp.maximum(pos, 0)
    at_top = pos // 32 >= length - 1
    low = jnp.where(at_top, length - 2, pos // 32)
    frac = jnp.where(at_top, 32, pos % 32)
    first, last = low[..., 0::2], low[..., 1::2] + 1
    owned = (first + last) // 2 // chip_rows == chip
    tile = first // tile_rows
    straddle = owned & (last // tile_rows > tile)

    def per_sample(a):
        return jnp.repeat(a, 2, axis=-1)

    edge = per_sample((tile + 1) * tile_rows)
    part_slot = 1 + BINS + per_sample(tile % 2)
    upper = per_sample(straddle) & (low >= edge)
    split = per_sample(straddle) & (low == edge - 1)
    start = chip * (chip_rows - HALO)
    side = right[..., None].astype(jnp.int32)
    live = per_sample(owned) & inside
    slot = jnp.where(upper, part_slot, 1 + jnp.arange(SAMPLES, dtype=jnp.int32) // 2)
    ids = jnp.arange(regions, dtype=jnp.int32)[:, None]
    gain = frac + jnp.where(split, GAINS, 0)
    keys = gain + (slot << 7) + (ids << 11) + ((2 * jnp.where(live, low - start, lists) + side) << 19)
    extra = []
    for q in range(2):
        here = split & live & per_sample(tile % 2 == q)
        number = lists - 2 + (q - chip) % 2
        key = jnp.max(jnp.where(here, frac + 2 * GAINS + ((1 + BINS + q) << 7) + (ids << 11) + ((2 * number + side) << 19), -1), axis=-1)
        extra.append(jnp.where(key < 0, (2 * lists) << 19, key))
    keys = jnp.concatenate([keys, jnp.stack(extra, axis=-1)], axis=-1)
    groups = keys.shape[0]
    number = keys >> 19
    ids = jnp.arange(16, dtype=jnp.int32)
    coarse = ((number >> 4)[..., None] == ids).astype(jnp.bfloat16)
    fine = ((number & 15)[..., None] == ids).astype(jnp.bfloat16)
    count = jnp.einsum('grka,grkb->gab', coarse, fine, preferred_element_type=jnp.float32).astype(jnp.int32).reshape(groups, 256)
    order = jnp.arange(256, dtype=jnp.int32)
    count = jnp.where(order < 2 * lists, count, 0)

    keys = lax.sort((keys + (jnp.arange(groups, dtype=jnp.int32) << 27)[:, None, None]).reshape(-1), is_stable=False)
    keys = jnp.pad(keys, (0, SPILL))
    region = (keys >> 11) & 255
    slots = region + ((keys >> 7) & 15) * 8 * (regions + SPARE)
    gains = (keys & 127) << 4

    blocks = (count + BLOCK - 1) // BLOCK
    earlier = order[:, None] < order[None, :]
    begin = jnp.sum(jnp.where(earlier, count[:, :, None], 0), axis=1)
    prior = jnp.sum(jnp.where(earlier, blocks[:, :, None], 0), axis=1)
    turn = jnp.arange(groups * plans, dtype=jnp.int32)
    column = order[:, None]

    def of(a):
        return jnp.where(turn < plans, a[0][:, None], a[1][:, None])

    turn_in = turn % plans
    nth = turn_in - 1 - of(prior)
    packed = column + (jnp.minimum(of(count) - BLOCK * nth, BLOCK) << 8) + ((of(begin) + BLOCK * nth) << 13)
    piece = turn_in - (plans - PIECES)
    reach = jnp.where(piece == PIECES - 1, 2 * lists, 2 * (chip * HALO + tile_rows // 2 * (piece + 1) - 1))
    chosen = jnp.where(piece < 0, jnp.where((nth >= 0) & (nth < of(blocks)), packed, 0), jnp.where(column < reach, of(blocks), 0))
    plan = jnp.sum(chosen, axis=0)

    bins = jnp.arange(BINS, dtype=jnp.int32) + 1
    joins = jnp.concatenate([jnp.sum(jnp.where(straddle & (tile % 2 == q), bins, 0), axis=-1) for q in range(2)], axis=0)
    return slots, gains, region, plan, joins


def list_sizes(regions, tile_rows):
    lists = 2 * tile_rows + HALO - 1 + 2
    plans = (regions * (SAMPLES + 2) + (BLOCK - 1) * 2 * lists) // BLOCK + TURNS + 4 + PIECES
    return lists, plans


def pool_kernel(dims, plan_ref, join_ref, slots_ref, gains_ref, tab_ats_ref, tabs_ref, own_ref, mate_ref, halo_ref, relay_ref, w_ref, out_ref,
                slot_ref, gain_ref, tab_at_ref, feat, tab_ref, acc_a, acc_b, gain, lhs, wbuf, fsem, hsem, tsem, lsem, wsem):
    group, tile_rows, feat_w, channels, regions = dims
    lists, plans = list_sizes(regions, tile_rows)
    me = lax.axis_index('sp')
    chip, core = me // 2, me % 2
    edge_one = tile_rows - 1 + chip * (tile_rows - 2 * tile_rows + HALO)
    edge_two = edge_one + tile_rows
    half = channels // 2
    row_in = BINS * channels
    first = chip * HALO
    some = tile_rows // 2

    def piece(source, q, part):
        return pltpu.make_async_copy(source.at[pl.ds(part * some, some)], feat.at[pl.ds(first + q * some, some)], fsem.at[q])

    def edge(source):
        return pltpu.make_async_copy(source, feat.at[pl.ds((1 - chip) * 2 * tile_rows, HALO)], hsem)

    columns = pltpu.make_async_copy(tabs_ref.at[group], tab_ref, tsem)
    columns.start()
    entries = slot_ref.shape[0]
    mine = pl.ds(group * (entries - SPILL), entries)
    entry_copies = [
        pltpu.make_async_copy(source.at[mine], target, lsem.at[i])
        for i, (source, target) in enumerate([(slots_ref, slot_ref), (gains_ref, gain_ref), (tab_ats_ref, tab_at_ref)])
    ]
    for copy in entry_copies:
        copy.start()

    @pl.when(chip != core)
    def _():
        edge(halo_ref).start()

    @pl.when(chip == core)
    def _():
        edge(relay_ref).start()

    @pl.when(core == 0)
    def _():
        for q, (source, part) in enumerate([(own_ref, 0), (own_ref, 1), (mate_ref, 0), (mate_ref, 1)]):
            piece(source, q, part).start()

    @pl.when(core == 1)
    def _():
        for q, (source, part) in enumerate([(mate_ref, 0), (mate_ref, 1), (own_ref, 0), (own_ref, 1)]):
            piece(source, q, part).start()

    depth = wbuf.shape[0]

    def weights(i):
        return pltpu.make_async_copy(w_ref.at[pl.ds(i * row_in, row_in)], wbuf.at[i % depth], wsem.at[i % depth])

    pitch = regions + SPARE
    zero = jnp.zeros((2 * pitch, half), jnp.float32)

    def clear(p, _):
        at = pl.ds(pl.multiple_of(p * 2 * pitch, 8), 2 * pitch)
        acc_a[at, :] = zero
        acc_b[at, :] = zero
        return 0

    lax.fori_loop(0, SLOTS * 4, clear, 0)

    def fill(f, _):
        high = jnp.full((8, half), f, jnp.int32).astype(jnp.float32) / 64.0
        for kind in range(3):
            at = pl.multiple_of((f + kind * GAINS) * 16, 16)
            gain[pl.ds(at, 8), :] = jnp.zeros_like(high) if kind == 2 else 0.5 - high
            gain[pl.ds(at + 8, 8), :] = jnp.zeros_like(high) if kind == 1 else high
        return 0

    lax.fori_loop(0, GAINS, fill, 0)

    def multiply(turn):
        plan = plan_ref[group * plans + turn]
        v = (plan & 255) >> 1
        column = pl.multiple_of((plan & 1) * (feat_w - WINDOW), 16)
        at = plan >> 13
        left = jnp.concatenate([tab_ref[tab_at_ref[at + s]] for s in range(BLOCK)], axis=0).astype(jnp.bfloat16)
        row = jnp.where(v < lists - 2, v, jnp.where(v == lists - 2, edge_one, edge_two))
        low = jnp.dot(left, feat[row, pl.ds(column, WINDOW), :], preferred_element_type=jnp.float32)
        high = jnp.dot(left, feat[row + 1, pl.ds(column, WINDOW), :], preferred_element_type=jnp.float32)
        return low, high

    def spread(turn, out):
        plan = plan_ref[group * plans + turn]
        live = (plan >> 8) & 31
        at = plan >> 13
        for s0 in range(0, BLOCK, 4):
            news = []
            for s in range(s0, s0 + 4):
                to = pl.ds(jnp.where(s < live, slot_ref[at + s], 0), 8, stride=pitch)
                weight = pl.multiple_of(gain_ref[at + s], 16)
                wl, wh = gain[pl.ds(weight, 8), :], gain[pl.ds(weight + 8, 8), :]
                for c, acc in enumerate((acc_a, acc_b)):
                    cols = slice(c * half, (c + 1) * half)
                    news.append((acc, to, acc[to, :] + (out[0][8 * s:8 * s + 8, cols] * wl + out[1][8 * s:8 * s + 8, cols] * wh)))
            for acc, to, value in news:
                acc[to, :] = value

    def turns(u, _):
        held = multiply(TURNS * u + 1)
        for t in range(1, TURNS):
            nxt = multiply(TURNS * u + t + 1)
            spread(TURNS * u + t, held)
            held = nxt
        spread(TURNS * u + TURNS, held)
        return 0

    columns.wait()
    for copy in entry_copies:
        copy.wait()
    edge(halo_ref).wait()

    def phase(q, done):
        piece(own_ref, q, 0).wait()

        @pl.when(q == PIECES - 1)
        def _():
            for i in range(depth):
                weights(i).start()

        bound = plan_ref[(group + 1) * plans - PIECES + q]
        upto = jnp.where(q == PIECES - 1, (bound + TURNS - 1) // TURNS, bound // TURNS)
        lax.fori_loop(done, upto, turns, 0)
        return upto

    done = lax.fori_loop(0, PIECES, phase, 0)

    def join(r4, _):
        news = []
        for r in range(4):
            for q in range(2):
                row = r4 * 4 + r
                to = pl.ds(row + join_ref[2 * q + group, row] * 8 * pitch, 8, stride=pitch)
                part = pl.ds(row + (1 + BINS + q) * 8 * pitch, 8, stride=pitch)
                for acc in (acc_a, acc_b):
                    news.append((acc, to, acc[to, :].astype(jnp.bfloat16).astype(jnp.float32) + acc[part, :].astype(jnp.bfloat16).astype(jnp.float32)))
        for acc, to, value in news:
            acc[to, :] = value
        return 0

    lax.fori_loop(0, regions // 4, join, 0)

    for i in range(BINS):
        for j in range(BINS):
            for c, acc in enumerate((acc_a, acc_b)):
                lhs[i % 2, :, j * channels + c * half:j * channels + (c + 1) * half] = acc[pl.ds(((1 + i) * 8 + j) * pitch, regions), :].astype(jnp.bfloat16)
        weights(i).wait()
        part = jnp.dot(lhs[i % 2], wbuf[i % depth], preferred_element_type=jnp.float32)
        if i == 0:
            out_ref[...] = part
        else:
            out_ref[...] += part
        if i + depth < BINS:
            weights(i + depth).start()


def pool_and_project(group, slots, gains, tab_at, plan, joins, tab, own, mate, halo, relay, w_one):
    tile_rows, feat_w, channels = own.shape
    regions = tab.shape[1]
    hidden = w_one.shape[1]
    row_in = BINS * channels
    entries = regions * (SAMPLES + 2) + SPILL
    depth = 3
    dims = (group, tile_rows, feat_w, channels, regions)
    smem = pl.BlockSpec(memory_space=pltpu.SMEM)
    vmem = pl.BlockSpec(memory_space=pltpu.VMEM)
    hbm = pl.BlockSpec(memory_space=pl.ANY)
    return pl.pallas_call(
        functools.partial(pool_kernel, dims),
        out_shape=jax.ShapeDtypeStruct((regions, hidden), jnp.float32),
        in_specs=[smem] * 2 + [hbm] * 9,
        out_specs=vmem,
        scratch_shapes=[
            pltpu.SMEM((entries,), jnp.int32),
            pltpu.SMEM((entries,), jnp.int32),
            pltpu.SMEM((entries,), jnp.int32),
            pltpu.VMEM((2 * tile_rows + HALO, feat_w, channels), jnp.bfloat16),
            pltpu.VMEM(tab.shape[1:], jnp.float32),
            pltpu.VMEM((SLOTS * 8 * (regions + SPARE), channels // 2), jnp.float32),
            pltpu.VMEM((SLOTS * 8 * (regions + SPARE), channels // 2), jnp.float32),
            pltpu.VMEM((3 * GAINS * 16, channels // 2), jnp.float32),
            pltpu.VMEM((2, regions, row_in), jnp.bfloat16),
            pltpu.VMEM((depth, row_in, hidden), jnp.bfloat16),
            pltpu.SemaphoreType.DMA((PIECES,)),
            pltpu.SemaphoreType.DMA(()),
            pltpu.SemaphoreType.DMA(()),
            pltpu.SemaphoreType.DMA((3,)),
            pltpu.SemaphoreType.DMA((depth,)),
        ],
        compiler_params=pltpu.CompilerParams(vmem_limit_bytes=64 * 1024 * 1024 - 65536),
        cost_estimate=pl.CostEstimate(flops=30_000_000_000, bytes_accessed=50_000_000, transcendentals=0),
        name='pool',
    )(plan, joins, slots, gains, tab_at, tab, own, mate, halo, relay, w_one)


def solution(mesh):
    group = mesh.shape['sp']

    def device_step(feature_map, box_coords, w_one, b_one, w_two, b_two):
        tile_rows, feat_w, channels = feature_map.shape
        regions = box_coords.shape[0] // group
        me = lax.axis_index('sp')
        chip, core = me // 2, me % 2

        mate = lax.ppermute(feature_map, 'sp', [(0, 1), (1, 0), (2, 3), (3, 2)])
        rim = jnp.where(core == 1, feature_map[tile_rows - HALO:], feature_map[:HALO])
        hop_one = lax.ppermute(rim, 'sp', [(1, 2), (2, 1)])
        hop_two = lax.ppermute(hop_one, 'sp', [(1, 0), (2, 3)])

        far = (me + 2) % 4
        boxes = jnp.stack([lax.dynamic_slice_in_dim(box_coords, g * regions, regions, 0) for g in (far, me)])
        tab, right = column_table(boxes, feat_w)
        lists = row_lists(boxes, right, chip, tile_rows, tile_rows * group)

        def project(g):
            return pool_and_project(g, *lists, tab, feature_map, mate, hop_one, hop_two, w_one)

        away = project(0)
        back = lax.ppermute(away, 'sp', [(0, 2), (2, 0), (1, 3), (3, 1)])
        here = project(1)
        hidden_act = jnp.maximum(here + back + b_one, 0.0).astype(jnp.bfloat16)
        return jnp.maximum(jnp.dot(hidden_act, w_two, preferred_element_type=jnp.float32) + b_two, 0.0).astype(jnp.bfloat16)

    return jax.shard_map(device_step, mesh=mesh, in_specs=(P(('dp', 'sp'), None, None), P('dp', None), P(), P(), P(), P()), out_specs=P(('dp', 'sp'), None), check_vma=False)
```

```python
import functools

import jax
import jax.numpy as jnp
from jax import lax
from jax.experimental import pallas as pl
from jax.experimental.pallas import tpu as pltpu
from jax.sharding import PartitionSpec as P

BINS = 7
SAMPLES = 2 * BINS
HALO = 6
WINDOW = 256
BLOCK = 16
GAINS = 33
SPILL = 1024
TURNS = 12
PIECES = 4
SLOTS = 10
SPARE = 2


def sample_rows(start_eighths, span_units, length):
    ids = jnp.arange(SAMPLES, dtype=jnp.int32)
    pos = 4 * start_eighths[..., None] - 16 + (2 * ids + 1) * span_units[..., None]
    inside = (pos >= -32) & (pos <= 32 * length)
    return pos, inside


def column_table(boxes, feat_w):
    start, span = boxes[..., 1, None], (boxes[..., 3, None] - boxes[..., 1, None]) // 7
    right = jnp.maximum(4 * start - 16 + span, 0) // 32 >= feat_w - WINDOW
    shift = jnp.where(right, feat_w - WINDOW, 0)
    ids = jnp.arange(BINS + 1, dtype=jnp.int32)
    cols = lax.broadcasted_iota(jnp.float32, start.shape[:-1] + (BINS + 1, WINDOW), start.ndim)

    def tent(which):
        pos = 4 * start - 16 + (4 * ids + 2 * which + 1) * span
        inside = (pos >= -32) & (pos <= 32 * feat_w) & (ids < BINS)
        at = (jnp.clip(pos, 0, 32 * (feat_w - 1)) - 32 * shift).astype(jnp.float32) / 32.0
        return jnp.maximum(1.0 - jnp.abs(cols - jnp.where(inside, at, -4.0)[..., None]), 0.0)

    return (tent(0) + tent(1)) * 0.5, right[..., 0]


def row_lists(boxes, right, chip, tile_rows, length):
    regions = boxes.shape[-2]
    chip_rows = 2 * tile_rows
    lists, plans = list_sizes(regions, tile_rows)
    pos, inside = sample_rows(boxes[..., 0], (boxes[..., 2] - boxes[..., 0]) // 7, length)
    pos = jnp.maximum(pos, 0)
    at_top = pos // 32 >= length - 1
    low = jnp.where(at_top, length - 2, pos // 32)
    frac = jnp.where(at_top, 32, pos % 32)
    first, last = low[..., 0::2], low[..., 1::2] + 1
    owned = (first + last) // 2 // chip_rows == chip
    tile = first // tile_rows
    straddle = owned & (last // tile_rows > tile)

    def per_sample(a):
        return jnp.repeat(a, 2, axis=-1)

    edge = per_sample((tile + 1) * tile_rows)
    part_slot = 1 + BINS + per_sample(tile % 2)
    upper = per_sample(straddle) & (low >= edge)
    split = per_sample(straddle) & (low == edge - 1)
    start = chip * (chip_rows - HALO)
    side = right[..., None].astype(jnp.int32)
    live = per_sample(owned) & inside
    slot = jnp.where(upper, part_slot, 1 + jnp.arange(SAMPLES, dtype=jnp.int32) // 2)
    ids = jnp.arange(regions, dtype=jnp.int32)[:, None]
    gain = frac + jnp.where(split, GAINS, 0)
    keys = gain + (slot << 7) + (ids << 11) + ((2 * jnp.where(live, low - start, lists) + side) << 19)
    extra = []
    for q in range(2):
        here = split & live & per_sample(tile % 2 == q)
        number = lists - 2 + (q - chip) % 2
        key = jnp.max(jnp.where(here, frac + 2 * GAINS + ((1 + BINS + q) << 7) + (ids << 11) + ((2 * number + side) << 19), -1), axis=-1)
        extra.append(jnp.where(key < 0, (2 * lists) << 19, key))
    keys = jnp.concatenate([keys, jnp.stack(extra, axis=-1)], axis=-1)
    groups = keys.shape[0]
    number = keys >> 19
    ids = jnp.arange(16, dtype=jnp.int32)
    coarse = ((number >> 4)[..., None] == ids).astype(jnp.bfloat16)
    fine = ((number & 15)[..., None] == ids).astype(jnp.bfloat16)
    count = jnp.einsum('grka,grkb->gab', coarse, fine, preferred_element_type=jnp.float32).astype(jnp.int32).reshape(groups, 256)
    order = jnp.arange(256, dtype=jnp.int32)
    count = jnp.where(order < 2 * lists, count, 0)

    keys = lax.sort((keys + (jnp.arange(groups, dtype=jnp.int32) << 27)[:, None, None]).reshape(-1), is_stable=False)
    keys = jnp.pad(keys, (0, SPILL))
    region = (keys >> 11) & 255
    slots = region + ((keys >> 7) & 15) * 16 * (regions + SPARE)
    gains = (keys & 127) << 4

    blocks = (count + BLOCK - 1) // BLOCK
    earlier = order[:, None] < order[None, :]
    begin = jnp.sum(jnp.where(earlier, count[:, :, None], 0), axis=1)
    prior = jnp.sum(jnp.where(earlier, blocks[:, :, None], 0), axis=1)
    turn = jnp.arange(groups * plans, dtype=jnp.int32)
    column = order[:, None]

    def of(a):
        return jnp.where(turn < plans, a[0][:, None], a[1][:, None])

    turn_in = turn % plans
    nth = turn_in - 1 - of(prior)
    packed = column + (jnp.minimum(of(count) - BLOCK * nth, BLOCK) << 8) + ((of(begin) + BLOCK * nth) << 13)
    piece = turn_in - (plans - PIECES)
    reach = jnp.where(piece == PIECES - 1, 2 * lists, 2 * (chip * HALO + tile_rows // 2 * (piece + 1) - 1))
    chosen = jnp.where(piece < 0, jnp.where((nth >= 0) & (nth < of(blocks)), packed, 0), jnp.where(column < reach, of(blocks), 0))
    plan = jnp.sum(chosen, axis=0)

    bins = jnp.arange(BINS, dtype=jnp.int32) + 1
    joins = jnp.concatenate([jnp.sum(jnp.where(straddle & (tile % 2 == q), bins, 0), axis=-1) for q in range(2)], axis=0)
    return slots, gains, region, plan, joins


def list_sizes(regions, tile_rows):
    lists = 2 * tile_rows + HALO - 1 + 2
    plans = (regions * (SAMPLES + 2) + (BLOCK - 1) * 2 * lists) // BLOCK + TURNS + 4 + PIECES
    return lists, plans


def pool_kernel(dims, plan_ref, join_ref, slots_ref, gains_ref, tab_ats_ref, tabs_ref, own_ref, mate_ref, halo_ref, relay_ref, w_ref, out_ref,
                slot_ref, gain_ref, tab_at_ref, feat, tab_ref, acc, gain, lhs, wbuf, fsem, hsem, tsem, lsem, wsem):
    group, tile_rows, feat_w, channels, regions = dims
    lists, plans = list_sizes(regions, tile_rows)
    me = lax.axis_index('sp')
    chip, core = me // 2, me % 2
    edge_one = tile_rows - 1 + chip * (tile_rows - 2 * tile_rows + HALO)
    edge_two = edge_one + tile_rows
    half = channels // 2
    row_in = BINS * channels
    first = chip * HALO
    some = tile_rows // 2

    def piece(source, q, part):
        return pltpu.make_async_copy(source.at[pl.ds(part * some, some)], feat.at[pl.ds(first + q * some, some)], fsem.at[q])

    def edge(source):
        return pltpu.make_async_copy(source, feat.at[pl.ds((1 - chip) * 2 * tile_rows, HALO)], hsem)

    columns = pltpu.make_async_copy(tabs_ref.at[group], tab_ref, tsem)
    columns.start()
    entries = slot_ref.shape[0]
    mine = pl.ds(group * (entries - SPILL), entries)
    entry_copies = [
        pltpu.make_async_copy(source.at[mine], target, lsem.at[i])
        for i, (source, target) in enumerate([(slots_ref, slot_ref), (gains_ref, gain_ref), (tab_ats_ref, tab_at_ref)])
    ]
    for copy in entry_copies:
        copy.start()

    @pl.when(chip != core)
    def _():
        edge(halo_ref).start()

    @pl.when(chip == core)
    def _():
        edge(relay_ref).start()

    @pl.when(core == 0)
    def _():
        for q, (source, part) in enumerate([(own_ref, 0), (own_ref, 1), (mate_ref, 0), (mate_ref, 1)]):
            piece(source, q, part).start()

    @pl.when(core == 1)
    def _():
        for q, (source, part) in enumerate([(mate_ref, 0), (mate_ref, 1), (own_ref, 0), (own_ref, 1)]):
            piece(source, q, part).start()

    depth = wbuf.shape[0]

    def weights(i):
        return pltpu.make_async_copy(w_ref.at[pl.ds(i * row_in, row_in)], wbuf.at[i % depth], wsem.at[i % depth])

    pitch = regions + SPARE
    zero = jnp.zeros((4 * pitch, half), jnp.float32)

    def clear(p, _):
        acc[pl.ds(pl.multiple_of(p * 4 * pitch, 8), 4 * pitch), :] = zero
        return 0

    lax.fori_loop(0, SLOTS * 4, clear, 0)

    def fill(f, _):
        high = jnp.full((8, half), f, jnp.int32).astype(jnp.float32) / 64.0
        for kind in range(3):
            at = pl.multiple_of((f + kind * GAINS) * 16, 16)
            gain[pl.ds(at, 8), :] = jnp.zeros_like(high) if kind == 2 else 0.5 - high
            gain[pl.ds(at + 8, 8), :] = jnp.zeros_like(high) if kind == 1 else high
        return 0

    lax.fori_loop(0, GAINS, fill, 0)

    def multiply(turn):
        plan = plan_ref[group * plans + turn]
        v = (plan & 255) >> 1
        column = pl.multiple_of((plan & 1) * (feat_w - WINDOW), 16)
        at = plan >> 13
        left = jnp.concatenate([tab_ref[tab_at_ref[at + s]] for s in range(BLOCK)], axis=0).astype(jnp.bfloat16)
        row = jnp.where(v < lists - 2, v, jnp.where(v == lists - 2, edge_one, edge_two))
        low = jnp.dot(left, feat[row, pl.ds(column, WINDOW), :], preferred_element_type=jnp.float32)
        high = jnp.dot(left, feat[row + 1, pl.ds(column, WINDOW), :], preferred_element_type=jnp.float32)
        return low, high

    def spread(turn, out):
        plan = plan_ref[group * plans + turn]
        live = (plan >> 8) & 31
        at = plan >> 13
        for s0 in range(0, BLOCK, 4):
            news = []
            for s in range(s0, s0 + 4):
                slot = jnp.where(s < live, slot_ref[at + s], 0)
                weight = pl.multiple_of(gain_ref[at + s], 16)
                wl, wh = gain[pl.ds(weight, 8), :], gain[pl.ds(weight + 8, 8), :]
                for c in range(2):
                    cols = slice(c * half, (c + 1) * half)
                    to = pl.ds(slot + c * pitch, 8, stride=2 * pitch)
                    news.append((to, acc[to, :] + (out[0][8 * s:8 * s + 8, cols] * wl + out[1][8 * s:8 * s + 8, cols] * wh)))
            for to, value in news:
                acc[to, :] = value

    def turns(u, _):
        held = multiply(TURNS * u + 1)
        for t in range(1, TURNS):
            nxt = multiply(TURNS * u + t + 1)
            spread(TURNS * u + t, held)
            held = nxt
        spread(TURNS * u + TURNS, held)
        return 0

    columns.wait()
    for copy in entry_copies:
        copy.wait()
    edge(halo_ref).wait()

    def phase(q, done):
        piece(own_ref, q, 0).wait()

        @pl.when(q == PIECES - 1)
        def _():
            for i in range(depth):
                weights(i).start()

        bound = plan_ref[(group + 1) * plans - PIECES + q]
        upto = jnp.where(q == PIECES - 1, (bound + TURNS - 1) // TURNS, bound // TURNS)
        lax.fori_loop(done, upto, turns, 0)
        return upto

    done = lax.fori_loop(0, PIECES, phase, 0)

    def join(r4, _):
        news = []
        for r in range(4):
            for q in range(2):
                row = r4 * 4 + r
                joined = row + join_ref[2 * q + group, row] * 16 * pitch
                for c in range(2):
                    to = pl.ds(joined + c * pitch, 8, stride=2 * pitch)
                    part = pl.ds(row + ((1 + BINS + q) * 16 + c) * pitch, 8, stride=2 * pitch)
                    news.append((to, acc[to, :].astype(jnp.bfloat16).astype(jnp.float32) + acc[part, :].astype(jnp.bfloat16).astype(jnp.float32)))
        for to, value in news:
            acc[to, :] = value
        return 0

    lax.fori_loop(0, regions // 4, join, 0)

    for i in range(BINS):
        for j in range(BINS):
            for c in range(2):
                lhs[i % 2, :, j * channels + c * half:j * channels + (c + 1) * half] = acc[pl.ds(((1 + i) * 16 + 2 * j + c) * pitch, regions), :].astype(jnp.bfloat16)
        weights(i).wait()
        part = jnp.dot(lhs[i % 2], wbuf[i % depth], preferred_element_type=jnp.float32)
        if i == 0:
            out_ref[...] = part
        else:
            out_ref[...] += part
        if i + depth < BINS:
            weights(i + depth).start()


def pool_and_project(group, slots, gains, tab_at, plan, joins, tab, own, mate, halo, relay, w_one):
    tile_rows, feat_w, channels = own.shape
    regions = tab.shape[1]
    hidden = w_one.shape[1]
    row_in = BINS * channels
    entries = regions * (SAMPLES + 2) + SPILL
    depth = 3
    dims = (group, tile_rows, feat_w, channels, regions)
    smem = pl.BlockSpec(memory_space=pltpu.SMEM)
    vmem = pl.BlockSpec(memory_space=pltpu.VMEM)
    hbm = pl.BlockSpec(memory_space=pl.ANY)
    return pl.pallas_call(
        functools.partial(pool_kernel, dims),
        out_shape=jax.ShapeDtypeStruct((regions, hidden), jnp.float32),
        in_specs=[smem] * 2 + [hbm] * 9,
        out_specs=vmem,
        scratch_shapes=[
            pltpu.SMEM((entries,), jnp.int32),
            pltpu.SMEM((entries,), jnp.int32),
            pltpu.SMEM((entries,), jnp.int32),
            pltpu.VMEM((2 * tile_rows + HALO, feat_w, channels), jnp.bfloat16),
            pltpu.VMEM(tab.shape[1:], jnp.float32),
            pltpu.VMEM((SLOTS * 16 * (regions + SPARE), channels // 2), jnp.float32),
            pltpu.VMEM((3 * GAINS * 16, channels // 2), jnp.float32),
            pltpu.VMEM((2, regions, row_in), jnp.bfloat16),
            pltpu.VMEM((depth, row_in, hidden), jnp.bfloat16),
            pltpu.SemaphoreType.DMA((PIECES,)),
            pltpu.SemaphoreType.DMA(()),
            pltpu.SemaphoreType.DMA(()),
            pltpu.SemaphoreType.DMA((3,)),
            pltpu.SemaphoreType.DMA((depth,)),
        ],
        compiler_params=pltpu.CompilerParams(vmem_limit_bytes=64 * 1024 * 1024 - 65536),
        cost_estimate=pl.CostEstimate(flops=30_000_000_000, bytes_accessed=50_000_000, transcendentals=0),
        name='pool',
    )(plan, joins, slots, gains, tab_at, tab, own, mate, halo, relay, w_one)


def solution(mesh):
    group = mesh.shape['sp']

    def device_step(feature_map, box_coords, w_one, b_one, w_two, b_two):
        tile_rows, feat_w, channels = feature_map.shape
        regions = box_coords.shape[0] // group
        me = lax.axis_index('sp')
        chip, core = me // 2, me % 2

        mate = lax.ppermute(feature_map, 'sp', [(0, 1), (1, 0), (2, 3), (3, 2)])
        rim = jnp.where(core == 1, feature_map[tile_rows - HALO:], feature_map[:HALO])
        hop_one = lax.ppermute(rim, 'sp', [(1, 2), (2, 1)])
        hop_two = lax.ppermute(hop_one, 'sp', [(1, 0), (2, 3)])

        far = (me + 2) % 4
        boxes = jnp.stack([lax.dynamic_slice_in_dim(box_coords, g * regions, regions, 0) for g in (far, me)])
        tab, right = column_table(boxes, feat_w)
        lists = row_lists(boxes, right, chip, tile_rows, tile_rows * group)

        def project(g):
            return pool_and_project(g, *lists, tab, feature_map, mate, hop_one, hop_two, w_one)

        away = project(0)
        back = lax.ppermute(away, 'sp', [(0, 2), (2, 0), (1, 3), (3, 1)])
        here = project(1)
        hidden_act = jnp.maximum(here + back + b_one, 0.0).astype(jnp.bfloat16)
        return jnp.maximum(jnp.dot(hidden_act, w_two, preferred_element_type=jnp.float32) + b_two, 0.0).astype(jnp.bfloat16)

    return jax.shard_map(device_step, mesh=mesh, in_specs=(P(('dp', 'sp'), None, None), P('dp', None), P(), P(), P(), P()), out_specs=P(('dp', 'sp'), None), check_vma=False)
```

```python
import functools

import jax
import jax.numpy as jnp
from jax import lax
from jax.experimental import pallas as pl
from jax.experimental.pallas import tpu as pltpu
from jax.sharding import PartitionSpec as P

BINS = 7
SAMPLES = 2 * BINS
HALO = 6
WINDOW = 256
BLOCK = 16
GAINS = 33
SPILL = 1024
TURNS = 16
PIECES = 4
SLOTS = 10
SPARE = 2


def sample_rows(start_eighths, span_units, length):
    ids = jnp.arange(SAMPLES, dtype=jnp.int32)
    pos = 4 * start_eighths[..., None] - 16 + (2 * ids + 1) * span_units[..., None]
    inside = (pos >= -32) & (pos <= 32 * length)
    return pos, inside


def column_table(boxes, feat_w):
    start, span = boxes[..., 1, None], (boxes[..., 3, None] - boxes[..., 1, None]) // 7
    right = jnp.maximum(4 * start - 16 + span, 0) // 32 >= feat_w - WINDOW
    shift = jnp.where(right, feat_w - WINDOW, 0)
    ids = jnp.arange(BINS + 1, dtype=jnp.int32)
    cols = lax.broadcasted_iota(jnp.float32, start.shape[:-1] + (BINS + 1, WINDOW), start.ndim)

    def tent(which):
        pos = 4 * start - 16 + (4 * ids + 2 * which + 1) * span
        inside = (pos >= -32) & (pos <= 32 * feat_w) & (ids < BINS)
        at = (jnp.clip(pos, 0, 32 * (feat_w - 1)) - 32 * shift).astype(jnp.float32) / 32.0
        return jnp.maximum(1.0 - jnp.abs(cols - jnp.where(inside, at, -4.0)[..., None]), 0.0)

    return (tent(0) + tent(1)) * 0.5, right[..., 0]


def row_lists(boxes, right, chip, tile_rows, length):
    regions = boxes.shape[-2]
    chip_rows = 2 * tile_rows
    lists, plans = list_sizes(regions, tile_rows)
    pos, inside = sample_rows(boxes[..., 0], (boxes[..., 2] - boxes[..., 0]) // 7, length)
    pos = jnp.maximum(pos, 0)
    at_top = pos // 32 >= length - 1
    low = jnp.where(at_top, length - 2, pos // 32)
    frac = jnp.where(at_top, 32, pos % 32)
    first, last = low[..., 0::2], low[..., 1::2] + 1
    owned = (first + last) // 2 // chip_rows == chip
    tile = first // tile_rows
    straddle = owned & (last // tile_rows > tile)

    def per_sample(a):
        return jnp.repeat(a, 2, axis=-1)

    edge = per_sample((tile + 1) * tile_rows)
    part_slot = 1 + BINS + per_sample(tile % 2)
    upper = per_sample(straddle) & (low >= edge)
    split = per_sample(straddle) & (low == edge - 1)
    start = chip * (chip_rows - HALO)
    side = right[..., None].astype(jnp.int32)
    live = per_sample(owned) & inside
    slot = jnp.where(upper, part_slot, 1 + jnp.arange(SAMPLES, dtype=jnp.int32) // 2)
    ids = jnp.arange(regions, dtype=jnp.int32)[:, None]
    gain = frac + jnp.where(split, GAINS, 0)
    keys = gain + (slot << 7) + (ids << 11) + ((2 * jnp.where(live, low - start, lists) + side) << 19)
    extra = []
    for q in range(2):
        here = split & live & per_sample(tile % 2 == q)
        number = lists - 2 + (q - chip) % 2
        key = jnp.max(jnp.where(here, frac + 2 * GAINS + ((1 + BINS + q) << 7) + (ids << 11) + ((2 * number + side) << 19), -1), axis=-1)
        extra.append(jnp.where(key < 0, (2 * lists) << 19, key))
    keys = jnp.concatenate([keys, jnp.stack(extra, axis=-1)], axis=-1)
    groups = keys.shape[0]
    number = keys >> 19
    ids = jnp.arange(16, dtype=jnp.int32)
    coarse = ((number >> 4)[..., None] == ids).astype(jnp.bfloat16)
    fine = ((number & 15)[..., None] == ids).astype(jnp.bfloat16)
    count = jnp.einsum('grka,grkb->gab', coarse, fine, preferred_element_type=jnp.float32).astype(jnp.int32).reshape(groups, 256)
    order = jnp.arange(256, dtype=jnp.int32)
    count = jnp.where(order < 2 * lists, count, 0)

    keys = lax.sort((keys + (jnp.arange(groups, dtype=jnp.int32) << 27)[:, None, None]).reshape(-1), is_stable=False)
    keys = jnp.pad(keys, (0, SPILL))
    region = (keys >> 11) & 255
    slots = region + ((keys >> 7) & 15) * 16 * (regions + SPARE)
    gains = (keys & 127) << 4

    blocks = (count + BLOCK - 1) // BLOCK
    earlier = order[:, None] < order[None, :]
    begin = jnp.sum(jnp.where(earlier, count[:, :, None], 0), axis=1)
    prior = jnp.sum(jnp.where(earlier, blocks[:, :, None], 0), axis=1)
    turn = jnp.arange(groups * plans, dtype=jnp.int32)
    column = order[:, None]

    def of(a):
        return jnp.where(turn < plans, a[0][:, None], a[1][:, None])

    turn_in = turn % plans
    nth = turn_in - 1 - of(prior)
    packed = column + (jnp.minimum(of(count) - BLOCK * nth, BLOCK) << 8) + ((of(begin) + BLOCK * nth) << 13)
    piece = turn_in - (plans - PIECES)
    reach = jnp.where(piece == PIECES - 1, 2 * lists, 2 * (chip * HALO + tile_rows // 2 * (piece + 1) - 1))
    chosen = jnp.where(piece < 0, jnp.where((nth >= 0) & (nth < of(blocks)), packed, 0), jnp.where(column < reach, of(blocks), 0))
    plan = jnp.sum(chosen, axis=0)

    bins = jnp.arange(BINS, dtype=jnp.int32) + 1
    joins = jnp.concatenate([jnp.sum(jnp.where(straddle & (tile % 2 == q), bins, 0), axis=-1) for q in range(2)], axis=0)
    return slots, gains, region, plan, joins


def list_sizes(regions, tile_rows):
    lists = 2 * tile_rows + HALO - 1 + 2
    plans = (regions * (SAMPLES + 2) + (BLOCK - 1) * 2 * lists) // BLOCK + TURNS + 4 + PIECES
    return lists, plans


def pool_kernel(dims, plan_ref, join_ref, slots_ref, gains_ref, tab_ats_ref, tabs_ref, own_ref, mate_ref, halo_ref, relay_ref, w_ref, out_ref,
                slot_ref, gain_ref, tab_at_ref, feat, tab_ref, acc, gain, lhs, wbuf, fsem, hsem, tsem, lsem, wsem):
    group, tile_rows, feat_w, channels, regions = dims
    lists, plans = list_sizes(regions, tile_rows)
    me = lax.axis_index('sp')
    chip, core = me // 2, me % 2
    edge_one = tile_rows - 1 + chip * (tile_rows - 2 * tile_rows + HALO)
    edge_two = edge_one + tile_rows
    half = channels // 2
    row_in = BINS * channels
    first = chip * HALO
    some = tile_rows // 2

    def piece(source, q, part):
        return pltpu.make_async_copy(source.at[pl.ds(part * some, some)], feat.at[pl.ds(first + q * some, some)], fsem.at[q])

    def edge(source):
        return pltpu.make_async_copy(source, feat.at[pl.ds((1 - chip) * 2 * tile_rows, HALO)], hsem)

    columns = pltpu.make_async_copy(tabs_ref.at[group], tab_ref, tsem)
    columns.start()
    entries = slot_ref.shape[0]
    mine = pl.ds(group * (entries - SPILL), entries)
    entry_copies = [
        pltpu.make_async_copy(source.at[mine], target, lsem.at[i])
        for i, (source, target) in enumerate([(slots_ref, slot_ref), (gains_ref, gain_ref), (tab_ats_ref, tab_at_ref)])
    ]
    for copy in entry_copies:
        copy.start()

    @pl.when(chip != core)
    def _():
        edge(halo_ref).start()

    @pl.when(chip == core)
    def _():
        edge(relay_ref).start()

    @pl.when(core == 0)
    def _():
        for q, (source, part) in enumerate([(own_ref, 0), (own_ref, 1), (mate_ref, 0), (mate_ref, 1)]):
            piece(source, q, part).start()

    @pl.when(core == 1)
    def _():
        for q, (source, part) in enumerate([(mate_ref, 0), (mate_ref, 1), (own_ref, 0), (own_ref, 1)]):
            piece(source, q, part).start()

    depth = wbuf.shape[0]

    def weights(i):
        return pltpu.make_async_copy(w_ref.at[pl.ds(i * row_in, row_in)], wbuf.at[i % depth], wsem.at[i % depth])

    pitch = regions + SPARE
    zero = jnp.zeros((4 * pitch, half), jnp.float32)

    def clear(p, _):
        acc[pl.ds(pl.multiple_of(p * 4 * pitch, 8), 4 * pitch), :] = zero
        return 0

    lax.fori_loop(0, SLOTS * 4, clear, 0)

    def fill(f, _):
        high = jnp.full((8, half), f, jnp.int32).astype(jnp.float32) / 64.0
        for kind in range(3):
            at = pl.multiple_of((f + kind * GAINS) * 16, 16)
            gain[pl.ds(at, 8), :] = jnp.zeros_like(high) if kind == 2 else 0.5 - high
            gain[pl.ds(at + 8, 8), :] = jnp.zeros_like(high) if kind == 1 else high
        return 0

    lax.fori_loop(0, GAINS, fill, 0)

    def multiply(turn):
        plan = plan_ref[group * plans + turn]
        v = (plan & 255) >> 1
        column = pl.multiple_of((plan & 1) * (feat_w - WINDOW), 16)
        at = plan >> 13
        left = jnp.concatenate([tab_ref[tab_at_ref[at + s]] for s in range(BLOCK)], axis=0).astype(jnp.bfloat16)
        row = jnp.where(v < lists - 2, v, jnp.where(v == lists - 2, edge_one, edge_two))
        low = jnp.dot(left, feat[row, pl.ds(column, WINDOW), :], preferred_element_type=jnp.float32)
        high = jnp.dot(left, feat[row + 1, pl.ds(column, WINDOW), :], preferred_element_type=jnp.float32)
        return low, high

    def spread(turn, out):
        plan = plan_ref[group * plans + turn]
        live = (plan >> 8) & 31
        at = plan >> 13
        for s0 in range(0, BLOCK, 4):
            news = []
            for s in range(s0, s0 + 4):
                slot = jnp.where(s < live, slot_ref[at + s], 0)
                weight = pl.multiple_of(gain_ref[at + s], 16)
                wl, wh = gain[pl.ds(weight, 8), :], gain[pl.ds(weight + 8, 8), :]
                for c in range(2):
                    cols = slice(c * half, (c + 1) * half)
                    to = pl.ds(slot + c * pitch, 8, stride=2 * pitch)
                    news.append((to, acc[to, :] + (out[0][8 * s:8 * s + 8, cols] * wl + out[1][8 * s:8 * s + 8, cols] * wh)))
            for to, value in news:
                acc[to, :] = value

    def turns(u, _):
        held = multiply(TURNS * u + 1)
        for t in range(1, TURNS):
            nxt = multiply(TURNS * u + t + 1)
            spread(TURNS * u + t, held)
            held = nxt
        spread(TURNS * u + TURNS, held)
        return 0

    columns.wait()
    for copy in entry_copies:
        copy.wait()
    edge(halo_ref).wait()

    def phase(q, done):
        piece(own_ref, q, 0).wait()

        @pl.when(q == PIECES - 1)
        def _():
            for i in range(depth):
                weights(i).start()

        bound = plan_ref[(group + 1) * plans - PIECES + q]
        upto = jnp.where(q == PIECES - 1, (bound + TURNS - 1) // TURNS, bound // TURNS)
        lax.fori_loop(done, upto, turns, 0)
        return upto

    done = lax.fori_loop(0, PIECES, phase, 0)

    def join(r8, _):
        news = []
        for r in range(8):
            for q in range(2):
                row = r8 * 8 + r
                joined = row + join_ref[2 * q + group, row] * 16 * pitch
                for c in range(2):
                    to = pl.ds(joined + c * pitch, 8, stride=2 * pitch)
                    part = pl.ds(row + ((1 + BINS + q) * 16 + c) * pitch, 8, stride=2 * pitch)
                    news.append((to, acc[to, :].astype(jnp.bfloat16).astype(jnp.float32) + acc[part, :].astype(jnp.bfloat16).astype(jnp.float32)))
        for to, value in news:
            acc[to, :] = value
        return 0

    lax.fori_loop(0, regions // 8, join, 0)

    for i in range(BINS):
        for j in range(BINS):
            for c in range(2):
                lhs[i % 2, :, j * channels + c * half:j * channels + (c + 1) * half] = acc[pl.ds(((1 + i) * 16 + 2 * j + c) * pitch, regions), :].astype(jnp.bfloat16)
        weights(i).wait()
        part = jnp.dot(lhs[i % 2], wbuf[i % depth], preferred_element_type=jnp.float32)
        if i == 0:
            out_ref[...] = part
        else:
            out_ref[...] += part
        if i + depth < BINS:
            weights(i + depth).start()


def pool_and_project(group, slots, gains, tab_at, plan, joins, tab, own, mate, halo, relay, w_one):
    tile_rows, feat_w, channels = own.shape
    regions = tab.shape[1]
    hidden = w_one.shape[1]
    row_in = BINS * channels
    entries = regions * (SAMPLES + 2) + SPILL
    depth = 3
    dims = (group, tile_rows, feat_w, channels, regions)
    smem = pl.BlockSpec(memory_space=pltpu.SMEM)
    vmem = pl.BlockSpec(memory_space=pltpu.VMEM)
    hbm = pl.BlockSpec(memory_space=pl.ANY)
    return pl.pallas_call(
        functools.partial(pool_kernel, dims),
        out_shape=jax.ShapeDtypeStruct((regions, hidden), jnp.float32),
        in_specs=[smem] * 2 + [hbm] * 9,
        out_specs=vmem,
        scratch_shapes=[
            pltpu.SMEM((entries,), jnp.int32),
            pltpu.SMEM((entries,), jnp.int32),
            pltpu.SMEM((entries,), jnp.int32),
            pltpu.VMEM((2 * tile_rows + HALO, feat_w, channels), jnp.bfloat16),
            pltpu.VMEM(tab.shape[1:], jnp.float32),
            pltpu.VMEM((SLOTS * 16 * (regions + SPARE), channels // 2), jnp.float32),
            pltpu.VMEM((3 * GAINS * 16, channels // 2), jnp.float32),
            pltpu.VMEM((2, regions, row_in), jnp.bfloat16),
            pltpu.VMEM((depth, row_in, hidden), jnp.bfloat16),
            pltpu.SemaphoreType.DMA((PIECES,)),
            pltpu.SemaphoreType.DMA(()),
            pltpu.SemaphoreType.DMA(()),
            pltpu.SemaphoreType.DMA((3,)),
            pltpu.SemaphoreType.DMA((depth,)),
        ],
        compiler_params=pltpu.CompilerParams(vmem_limit_bytes=64 * 1024 * 1024 - 65536),
        cost_estimate=pl.CostEstimate(flops=30_000_000_000, bytes_accessed=50_000_000, transcendentals=0),
        name='pool',
    )(plan, joins, slots, gains, tab_at, tab, own, mate, halo, relay, w_one)


def solution(mesh):
    group = mesh.shape['sp']

    def device_step(feature_map, box_coords, w_one, b_one, w_two, b_two):
        tile_rows, feat_w, channels = feature_map.shape
        regions = box_coords.shape[0] // group
        me = lax.axis_index('sp')
        chip, core = me // 2, me % 2

        mate = lax.ppermute(feature_map, 'sp', [(0, 1), (1, 0), (2, 3), (3, 2)])
        rim = lax.dynamic_slice_in_dim(feature_map, jnp.where(core == 1, tile_rows - HALO, 0), HALO, 0)
        hop_one = lax.ppermute(rim, 'sp', [(1, 2), (2, 1)])
        hop_two = lax.ppermute(hop_one, 'sp', [(1, 0), (2, 3)])

        far = (me + 2) % 4
        boxes = jnp.stack([lax.dynamic_slice_in_dim(box_coords, g * regions, regions, 0) for g in (far, me)])
        tab, right = column_table(boxes, feat_w)
        lists = row_lists(boxes, right, chip, tile_rows, tile_rows * group)

        def project(g):
            return pool_and_project(g, *lists, tab, feature_map, mate, hop_one, hop_two, w_one)

        away = project(0)
        back = lax.ppermute(away, 'sp', [(0, 2), (2, 0), (1, 3), (3, 1)])
        here = project(1)
        hidden_act = jnp.maximum(here + back + b_one, 0.0).astype(jnp.bfloat16)
        return jnp.maximum(jnp.dot(hidden_act, w_two, preferred_element_type=jnp.float32) + b_two, 0.0).astype(jnp.bfloat16)

    return jax.shard_map(device_step, mesh=mesh, in_specs=(P(('dp', 'sp'), None, None), P('dp', None), P(), P(), P(), P()), out_specs=P(('dp', 'sp'), None), check_vma=False)
```

```python
import functools

import jax
import jax.numpy as jnp
from jax import lax
from jax.experimental import pallas as pl
from jax.experimental.pallas import tpu as pltpu
from jax.sharding import PartitionSpec as P

BINS = 7
SAMPLES = 2 * BINS
HALO = 6
WINDOW = 256
BLOCK = 16
GAINS = 33
SPILL = 1024
TURNS = 20
PIECES = 4
SLOTS = 10
SPARE = 2


def sample_rows(start_eighths, span_units, length):
    ids = jnp.arange(SAMPLES, dtype=jnp.int32)
    pos = 4 * start_eighths[..., None] - 16 + (2 * ids + 1) * span_units[..., None]
    inside = (pos >= -32) & (pos <= 32 * length)
    return pos, inside


def column_table(boxes, feat_w):
    start, span = boxes[..., 1, None], (boxes[..., 3, None] - boxes[..., 1, None]) // 7
    right = jnp.maximum(4 * start - 16 + span, 0) // 32 >= feat_w - WINDOW
    shift = jnp.where(right, feat_w - WINDOW, 0)
    ids = jnp.arange(BINS + 1, dtype=jnp.int32)
    cols = lax.broadcasted_iota(jnp.float32, start.shape[:-1] + (BINS + 1, WINDOW), start.ndim)

    def tent(which):
        pos = 4 * start - 16 + (4 * ids + 2 * which + 1) * span
        inside = (pos >= -32) & (pos <= 32 * feat_w) & (ids < BINS)
        at = (jnp.clip(pos, 0, 32 * (feat_w - 1)) - 32 * shift).astype(jnp.float32) / 32.0
        return jnp.maximum(1.0 - jnp.abs(cols - jnp.where(inside, at, -4.0)[..., None]), 0.0)

    return (tent(0) + tent(1)) * 0.5, right[..., 0]


def row_lists(boxes, right, chip, tile_rows, length):
    regions = boxes.shape[-2]
    chip_rows = 2 * tile_rows
    lists, plans = list_sizes(regions, tile_rows)
    pos, inside = sample_rows(boxes[..., 0], (boxes[..., 2] - boxes[..., 0]) // 7, length)
    pos = jnp.maximum(pos, 0)
    at_top = pos // 32 >= length - 1
    low = jnp.where(at_top, length - 2, pos // 32)
    frac = jnp.where(at_top, 32, pos % 32)
    first, last = low[..., 0::2], low[..., 1::2] + 1
    owned = (first + last) // 2 // chip_rows == chip
    tile = first // tile_rows
    straddle = owned & (last // tile_rows > tile)

    def per_sample(a):
        return jnp.repeat(a, 2, axis=-1)

    edge = per_sample((tile + 1) * tile_rows)
    part_slot = 1 + BINS + per_sample(tile % 2)
    upper = per_sample(straddle) & (low >= edge)
    split = per_sample(straddle) & (low == edge - 1)
    start = chip * (chip_rows - HALO)
    side = right[..., None].astype(jnp.int32)
    live = per_sample(owned) & inside
    slot = jnp.where(upper, part_slot, 1 + jnp.arange(SAMPLES, dtype=jnp.int32) // 2)
    ids = jnp.arange(regions, dtype=jnp.int32)[:, None]
    gain = frac + jnp.where(split, GAINS, 0)
    keys = gain + (slot << 7) + (ids << 11) + ((2 * jnp.where(live, low - start, lists) + side) << 19)
    extra = []
    for q in range(2):
        here = split & live & per_sample(tile % 2 == q)
        number = lists - 2 + (q - chip) % 2
        key = jnp.max(jnp.where(here, frac + 2 * GAINS + ((1 + BINS + q) << 7) + (ids << 11) + ((2 * number + side) << 19), -1), axis=-1)
        extra.append(jnp.where(key < 0, (2 * lists) << 19, key))
    keys = jnp.concatenate([keys, jnp.stack(extra, axis=-1)], axis=-1)
    groups = keys.shape[0]
    number = keys >> 19
    ids = jnp.arange(16, dtype=jnp.int32)
    coarse = ((number >> 4)[..., None] == ids).astype(jnp.bfloat16)
    fine = ((number & 15)[..., None] == ids).astype(jnp.bfloat16)
    count = jnp.einsum('grka,grkb->gab', coarse, fine, preferred_element_type=jnp.float32).astype(jnp.int32).reshape(groups, 256)
    order = jnp.arange(256, dtype=jnp.int32)
    count = jnp.where(order < 2 * lists, count, 0)

    keys = lax.sort((keys + (jnp.arange(groups, dtype=jnp.int32) << 27)[:, None, None]).reshape(-1), is_stable=False)
    keys = jnp.pad(keys, (0, SPILL))
    region = (keys >> 11) & 255
    slots = region + ((keys >> 7) & 15) * 16 * (regions + SPARE)
    gains = (keys & 127) << 4

    blocks = (count + BLOCK - 1) // BLOCK
    earlier = order[:, None] < order[None, :]
    begin = jnp.sum(jnp.where(earlier, count[:, :, None], 0), axis=1)
    prior = jnp.sum(jnp.where(earlier, blocks[:, :, None], 0), axis=1)
    turn = jnp.arange(groups * plans, dtype=jnp.int32)
    column = order[:, None]

    def of(a):
        return jnp.where(turn < plans, a[0][:, None], a[1][:, None])

    turn_in = turn % plans
    nth = turn_in - 1 - of(prior)
    packed = column + (jnp.minimum(of(count) - BLOCK * nth, BLOCK) << 8) + ((of(begin) + BLOCK * nth) << 13)
    piece = turn_in - (plans - PIECES)
    reach = jnp.where(piece == PIECES - 1, 2 * lists, 2 * (chip * HALO + tile_rows // 2 * (piece + 1) - 1))
    chosen = jnp.where(piece < 0, jnp.where((nth >= 0) & (nth < of(blocks)), packed, 0), jnp.where(column < reach, of(blocks), 0))
    plan = jnp.sum(chosen, axis=0)

    bins = jnp.arange(BINS, dtype=jnp.int32) + 1
    joins = jnp.concatenate([jnp.sum(jnp.where(straddle & (tile % 2 == q), bins, 0), axis=-1) for q in range(2)], axis=0)
    return slots, gains, region, plan, joins


def list_sizes(regions, tile_rows):
    lists = 2 * tile_rows + HALO - 1 + 2
    plans = (regions * (SAMPLES + 2) + (BLOCK - 1) * 2 * lists) // BLOCK + TURNS + 4 + PIECES
    return lists, plans


def pool_kernel(dims, plan_ref, join_ref, slots_ref, gains_ref, tab_ats_ref, tabs_ref, own_ref, mate_ref, halo_ref, relay_ref, w_ref, out_ref,
                slot_ref, gain_ref, tab_at_ref, feat, tab_ref, acc, gain, lhs, wbuf, fsem, hsem, tsem, lsem, wsem):
    group, tile_rows, feat_w, channels, regions = dims
    lists, plans = list_sizes(regions, tile_rows)
    me = lax.axis_index('sp')
    chip, core = me // 2, me % 2
    edge_one = tile_rows - 1 + chip * (tile_rows - 2 * tile_rows + HALO)
    edge_two = edge_one + tile_rows
    half = channels // 2
    row_in = BINS * channels
    first = chip * HALO
    some = tile_rows // 2

    def piece(source, q, part):
        return pltpu.make_async_copy(source.at[pl.ds(part * some, some)], feat.at[pl.ds(first + q * some, some)], fsem.at[q])

    def edge(source):
        return pltpu.make_async_copy(source, feat.at[pl.ds((1 - chip) * 2 * tile_rows, HALO)], hsem)

    columns = pltpu.make_async_copy(tabs_ref.at[group], tab_ref, tsem)
    columns.start()
    entries = slot_ref.shape[0]
    mine = pl.ds(group * (entries - SPILL), entries)
    entry_copies = [
        pltpu.make_async_copy(source.at[mine], target, lsem.at[i])
        for i, (source, target) in enumerate([(slots_ref, slot_ref), (gains_ref, gain_ref), (tab_ats_ref, tab_at_ref)])
    ]
    for copy in entry_copies:
        copy.start()

    @pl.when(chip != core)
    def _():
        edge(halo_ref).start()

    @pl.when(chip == core)
    def _():
        edge(relay_ref).start()

    @pl.when(core == 0)
    def _():
        for q, (source, part) in enumerate([(own_ref, 0), (own_ref, 1), (mate_ref, 0), (mate_ref, 1)]):
            piece(source, q, part).start()

    @pl.when(core == 1)
    def _():
        for q, (source, part) in enumerate([(mate_ref, 0), (mate_ref, 1), (own_ref, 0), (own_ref, 1)]):
            piece(source, q, part).start()

    depth = wbuf.shape[0]

    def weights(i):
        return pltpu.make_async_copy(w_ref.at[pl.ds(i * row_in, row_in)], wbuf.at[i % depth], wsem.at[i % depth])

    pitch = regions + SPARE
    zero = jnp.zeros((4 * pitch, half), jnp.float32)

    def clear(p, _):
        acc[pl.ds(pl.multiple_of(p * 4 * pitch, 8), 4 * pitch), :] = zero
        return 0

    lax.fori_loop(0, SLOTS * 4, clear, 0)

    def fill(f, _):
        high = jnp.full((8, half), f, jnp.int32).astype(jnp.float32) / 64.0
        for kind in range(3):
            at = pl.multiple_of((f + kind * GAINS) * 16, 16)
            gain[pl.ds(at, 8), :] = jnp.zeros_like(high) if kind == 2 else 0.5 - high
            gain[pl.ds(at + 8, 8), :] = jnp.zeros_like(high) if kind == 1 else high
        return 0

    lax.fori_loop(0, GAINS, fill, 0)

    def multiply(turn):
        plan = plan_ref[group * plans + turn]
        v = (plan & 255) >> 1
        column = pl.multiple_of((plan & 1) * (feat_w - WINDOW), 16)
        at = plan >> 13
        left = jnp.concatenate([tab_ref[tab_at_ref[at + s]] for s in range(BLOCK)], axis=0).astype(jnp.bfloat16)
        row = jnp.where(v < lists - 2, v, jnp.where(v == lists - 2, edge_one, edge_two))
        low = jnp.dot(left, feat[row, pl.ds(column, WINDOW), :], preferred_element_type=jnp.float32)
        high = jnp.dot(left, feat[row + 1, pl.ds(column, WINDOW), :], preferred_element_type=jnp.float32)
        return low, high

    def spread(turn, out):
        plan = plan_ref[group * plans + turn]
        live = (plan >> 8) & 31
        at = plan >> 13
        for s0 in range(0, BLOCK, 4):
            news = []
            for s in range(s0, s0 + 4):
                slot = jnp.where(s < live, slot_ref[at + s], 0)
                weight = pl.multiple_of(gain_ref[at + s], 16)
                wl, wh = gain[pl.ds(weight, 8), :], gain[pl.ds(weight + 8, 8), :]
                for c in range(2):
                    cols = slice(c * half, (c + 1) * half)
                    to = pl.ds(slot + c * pitch, 8, stride=2 * pitch)
                    news.append((to, acc[to, :] + (out[0][8 * s:8 * s + 8, cols] * wl + out[1][8 * s:8 * s + 8, cols] * wh)))
            for to, value in news:
                acc[to, :] = value

    def turns(u, _):
        held = multiply(TURNS * u + 1)
        for t in range(1, TURNS):
            nxt = multiply(TURNS * u + t + 1)
            spread(TURNS * u + t, held)
            held = nxt
        spread(TURNS * u + TURNS, held)
        return 0

    columns.wait()
    for copy in entry_copies:
        copy.wait()
    edge(halo_ref).wait()

    def phase(q, done):
        piece(own_ref, q, 0).wait()

        @pl.when(q == PIECES - 1)
        def _():
            for i in range(depth):
                weights(i).start()

        bound = plan_ref[(group + 1) * plans - PIECES + q]
        upto = jnp.where(q == PIECES - 1, (bound + TURNS - 1) // TURNS, bound // TURNS)
        lax.fori_loop(done, upto, turns, 0)
        return upto

    done = lax.fori_loop(0, PIECES, phase, 0)

    def join(r8, _):
        news = []
        for r in range(8):
            for q in range(2):
                row = r8 * 8 + r
                joined = row + join_ref[2 * q + group, row] * 16 * pitch
                for c in range(2):
                    to = pl.ds(joined + c * pitch, 8, stride=2 * pitch)
                    part = pl.ds(row + ((1 + BINS + q) * 16 + c) * pitch, 8, stride=2 * pitch)
                    news.append((to, acc[to, :].astype(jnp.bfloat16).astype(jnp.float32) + acc[part, :].astype(jnp.bfloat16).astype(jnp.float32)))
        for to, value in news:
            acc[to, :] = value
        return 0

    lax.fori_loop(0, regions // 8, join, 0)

    for i in range(BINS):
        for j in range(BINS):
            for c in range(2):
                lhs[i % 2, :, j * channels + c * half:j * channels + (c + 1) * half] = acc[pl.ds(((1 + i) * 16 + 2 * j + c) * pitch, regions), :].astype(jnp.bfloat16)
        weights(i).wait()
        part = jnp.dot(lhs[i % 2], wbuf[i % depth], preferred_element_type=jnp.float32)
        if i == 0:
            out_ref[...] = part
        else:
            out_ref[...] += part
        if i + depth < BINS:
            weights(i + depth).start()


def pool_and_project(group, slots, gains, tab_at, plan, joins, tab, own, mate, halo, relay, w_one):
    tile_rows, feat_w, channels = own.shape
    regions = tab.shape[1]
    hidden = w_one.shape[1]
    row_in = BINS * channels
    entries = regions * (SAMPLES + 2) + SPILL
    depth = 3
    dims = (group, tile_rows, feat_w, channels, regions)
    smem = pl.BlockSpec(memory_space=pltpu.SMEM)
    vmem = pl.BlockSpec(memory_space=pltpu.VMEM)
    hbm = pl.BlockSpec(memory_space=pl.ANY)
    return pl.pallas_call(
        functools.partial(pool_kernel, dims),
        out_shape=jax.ShapeDtypeStruct((regions, hidden), jnp.float32),
        in_specs=[smem] * 2 + [hbm] * 9,
        out_specs=vmem,
        scratch_shapes=[
            pltpu.SMEM((entries,), jnp.int32),
            pltpu.SMEM((entries,), jnp.int32),
            pltpu.SMEM((entries,), jnp.int32),
            pltpu.VMEM((2 * tile_rows + HALO, feat_w, channels), jnp.bfloat16),
            pltpu.VMEM(tab.shape[1:], jnp.float32),
            pltpu.VMEM((SLOTS * 16 * (regions + SPARE), channels // 2), jnp.float32),
            pltpu.VMEM((3 * GAINS * 16, channels // 2), jnp.float32),
            pltpu.VMEM((2, regions, row_in), jnp.bfloat16),
            pltpu.VMEM((depth, row_in, hidden), jnp.bfloat16),
            pltpu.SemaphoreType.DMA((PIECES,)),
            pltpu.SemaphoreType.DMA(()),
            pltpu.SemaphoreType.DMA(()),
            pltpu.SemaphoreType.DMA((3,)),
            pltpu.SemaphoreType.DMA((depth,)),
        ],
        compiler_params=pltpu.CompilerParams(vmem_limit_bytes=64 * 1024 * 1024 - 65536),
        cost_estimate=pl.CostEstimate(flops=30_000_000_000, bytes_accessed=50_000_000, transcendentals=0),
        name='pool',
    )(plan, joins, slots, gains, tab_at, tab, own, mate, halo, relay, w_one)


def solution(mesh):
    group = mesh.shape['sp']

    def device_step(feature_map, box_coords, w_one, b_one, w_two, b_two):
        tile_rows, feat_w, channels = feature_map.shape
        regions = box_coords.shape[0] // group
        me = lax.axis_index('sp')
        chip, core = me // 2, me % 2

        mate = lax.ppermute(feature_map, 'sp', [(0, 1), (1, 0), (2, 3), (3, 2)])
        rim = lax.dynamic_slice_in_dim(feature_map, jnp.where(core == 1, tile_rows - HALO, 0), HALO, 0)
        hop_one = lax.ppermute(rim, 'sp', [(1, 2), (2, 1)])
        hop_two = lax.ppermute(hop_one, 'sp', [(1, 0), (2, 3)])

        far = (me + 2) % 4
        boxes = jnp.stack([lax.dynamic_slice_in_dim(box_coords, g * regions, regions, 0) for g in (far, me)])
        tab, right = column_table(boxes, feat_w)
        lists = row_lists(boxes, right, chip, tile_rows, tile_rows * group)

        def project(g):
            return pool_and_project(g, *lists, tab, feature_map, mate, hop_one, hop_two, w_one)

        away = project(0)
        back = lax.ppermute(away, 'sp', [(0, 2), (2, 0), (1, 3), (3, 1)])
        here = project(1)
        hidden_act = jnp.maximum(here + back + b_one, 0.0).astype(jnp.bfloat16)
        return jnp.maximum(jnp.dot(hidden_act, w_two, preferred_element_type=jnp.float32) + b_two, 0.0).astype(jnp.bfloat16)

    return jax.shard_map(device_step, mesh=mesh, in_specs=(P(('dp', 'sp'), None, None), P('dp', None), P(), P(), P(), P()), out_specs=P(('dp', 'sp'), None), check_vma=False)
```
